128 devices in a mesh: dp: 16 (over z, x), shard: 8 (over y, core).
Axes of the slice: x: 4, y: 4, z: 4, core: 2. Of those that a mesh axis runs over, the one named last changes fastest.
Arguments:
- tokens: bfloat16 [32768, 2048], P(('dp', 'shard')), may hold values from -24 to 24
- ctx_cotangent: bfloat16 [32768, 1024], P(('dp', 'shard')), may hold values from -0.59765625 to 0.59765625
- latent_cache: bfloat16 [2048, 128, 896], P('dp', 'shard'), may hold values from -300 to 300
- nbr_ids: int32 [512, 2], P(('dp', 'shard')), may hold values from 0 to 2047, as said below
- w_query: bfloat16 [2048, 1024], P('shard'), may hold values from -0.125 to 0.125
- w_key: bfloat16 [896, 1024], P('shard'), may hold values from -0.1875 to 0.1875
- w_value: bfloat16 [896, 1024], P('shard'), may hold values from -0.1875 to 0.1875
Outputs:
- context: bfloat16 [32768, 1024], P(('dp', 'shard'))
- grad_query: float32 [2048, 1024], P(('dp', 'shard'))
- grad_key: float32 [896, 1024], P(('dp', 'shard'))
- grad_value: float32 [896, 1024], P(('dp', 'shard'))
The draws below stay inside these ranges and needn't reach their ends.
Inputs may be any that keep to these rules, and one draw needn't show every extreme that they name: Row r of latent_cache is owned by index r // 128 of dp. Within the 64 ids of one index of dp (its devices' nbr_ids in row-major order), at most 8 name rows of one owner, and in every draw one owner is named exactly 8 times by every index of dp. Ids may repeat.
All inputs are finite; a program needn't handle non-finite values.
Results may differ from the reference program's by a relative error of at most 0.0055.
The reference program's roundings to bfloat16 on the way count: a program that leaves them out, or rounds other values in their place, can miss the bound.
Values may be sent and summed in bfloat16 or wider, within the bound.
A program may use at most 128 MiB of HBM per device.

```python
import jax
import jax.numpy as jnp
from jax import lax

D = 2048
LAT = 896
HEADS = 8
HEAD_DIM = 128
SPAN = 64
NBR = 2
NT = 128
CH_DEV = 4
ROW_DEV = 128
INNER = 1024
SPANS = 512
TOKENS = 32768
ROWS = 2048
GROUP = 64
CAP = 8
N_DP = 16
N_SHARD = 8


def draw_nbr_ids(key, part):
    owner_count = ROWS // ROW_DEV
    slot_total = owner_count * CAP
    hot_owner = jax.random.randint(jax.random.fold_in(key, 11), (), 0, owner_count)

    def one_group(index):
        group_key = jax.random.fold_in(jax.random.fold_in(key, 12), index)
        first_key, second_key, third_key = jax.random.split(group_key, 3)
        owner_of = jnp.arange(slot_total, dtype=jnp.int32) // CAP
        ranking = jax.random.permutation(first_key, slot_total).astype(jnp.int32)
        ranking = ranking - jnp.where(owner_of == hot_owner, slot_total, 0)
        ordering = jnp.argsort(ranking, stable=True)
        chosen = owner_of[ordering[:GROUP]]
        chosen = jax.random.permutation(second_key, chosen)
        within_row = jax.random.randint(third_key, (GROUP,), 0, ROW_DEV)
        return chosen * ROW_DEV + within_row
    group_count = SPANS * NBR // GROUP
    identities = jax.vmap(one_group)(jnp.arange(group_count))
    return identities.reshape(SPANS, NBR).astype(jnp.int32)


def draw_latent_cache(key, part):
    owner_count = ROWS // ROW_DEV
    base_key, pair_key = jax.random.split(jax.random.fold_in(key, 21), 2)
    values = jnp.clip(jax.random.normal(base_key, (ROWS, NT, LAT), jnp.float32), -6.0, 6.0)
    pairing = jax.random.permutation(pair_key, owner_count)
    owner_of = jnp.arange(ROWS) // ROW_DEV
    column_block = jnp.arange(LAT) * owner_count // LAT
    spiked = pairing[owner_of][:, None] == column_block[None, :]
    values = values * jnp.where(spiked, 4.0, 1.0)[:, None, :]
    return values.astype(jnp.bfloat16)


def raised(result, key, source, target, parts, factor):
    def block_of(axis_at):
        return (jnp.arange(result.shape[axis_at]) // (result.shape[axis_at] // parts)).reshape((-1,) + (1,) * (result.ndim - 1 - axis_at))

    one_side = jax.random.permutation(key, parts)[block_of(target)]
    second = (block_of(target) + parts // 2) % parts
    return jnp.where((block_of(source) == one_side) | (block_of(source) == second), factor * result, result)


def steps_of(stream_key, shape, cuts, least, top_value):
    def one(dim, blocks):
        draws = jax.random.uniform(jax.random.fold_in(jax.random.fold_in(stream_key, 6), dim), (blocks,), jnp.float32, least / len(cuts), top_value / len(cuts))
        return jnp.repeat(jnp.exp(draws), shape[dim] // blocks).reshape((-1,) + (1,) * (len(shape) - dim - 1))

    loudness = one(*cuts[0])
    for cut in cuts[1:]:
        loudness = loudness * one(*cut)
    return loudness


def bell_draw(stream_key, shape, deviation, reach, cuts=(), kind=jnp.bfloat16):
    values = deviation * jax.random.normal(stream_key, shape, jnp.float32)
    if cuts:
        values = values * steps_of(stream_key, shape, cuts, -0.22, 0.18)
    return jnp.clip(values, -reach, reach).astype(kind)


def noise_with(key, dims, deviation, limit, shards, heavy, kind=jnp.bfloat16):
    entries = deviation * jax.random.normal(key, dims, jnp.float32)
    if shards:
        entries = entries * steps_of(key, dims, shards, -0.22, 0.18)
    return jnp.clip(raised(entries, jax.random.fold_in(key, 3), *heavy), -limit, limit).astype(kind)


def setup_inputs(seed: int = 0) -> dict:
    arg_keys = jax.random.split(jax.random.key(seed), 8)
    tokens = noise_with(arg_keys[0], (TOKENS, D), 1.0, 24.0, ((0, 128),), (0, 1, 128, 5.5))
    ctx_cotangent = bell_draw(arg_keys[1], (TOKENS, INNER), 0.1, 0.59765625, ((0, 128),))
    latent_cache = draw_latent_cache(jax.random.fold_in(arg_keys[7], 71), 0)
    nbr_ids = draw_nbr_ids(jax.random.fold_in(arg_keys[7], 71), 0)
    w_query = bell_draw(arg_keys[4], (D, INNER), D ** -0.5, 0.125, ((0, 8),))
    w_key = bell_draw(arg_keys[5], (LAT, INNER), LAT ** -0.5, 0.1875, ((0, 8),))
    w_value = bell_draw(arg_keys[6], (LAT, INNER), LAT ** -0.5, 0.1875, ((0, 8),))
    return dict(tokens=tokens, ctx_cotangent=ctx_cotangent, latent_cache=latent_cache, nbr_ids=nbr_ids, w_query=w_query, w_key=w_key, w_value=w_value)


def attend_block(normed, latent_rows, ctx_grad, w_query, w_key, w_value):
    softmax_scale = HEAD_DIM ** (-0.5)
    query_sum = jnp.dot(normed, w_query, preferred_element_type=jnp.float32)
    queries = (query_sum * softmax_scale).astype(jnp.bfloat16)
    key_rows = jnp.dot(latent_rows, w_key, preferred_element_type=jnp.float32).astype(jnp.bfloat16)
    value_rows = jnp.dot(latent_rows, w_value, preferred_element_type=jnp.float32).astype(jnp.bfloat16)
    query_heads = queries.reshape(CH_DEV, SPAN, HEADS, HEAD_DIM).astype(jnp.float32)
    key_heads = key_rows.reshape(CH_DEV, NBR * NT, HEADS, HEAD_DIM).astype(jnp.float32)
    value_heads = value_rows.reshape(CH_DEV, NBR * NT, HEADS, HEAD_DIM).astype(jnp.float32)
    scores = jnp.einsum('cmhd,cnhd->chmn', query_heads, key_heads)
    highest = lax.optimization_barrier(jnp.max(scores, axis=-1, keepdims=True))
    exp_scores = jnp.exp(scores - highest)
    attn_prob = exp_scores / lax.optimization_barrier(jnp.sum(exp_scores, axis=-1, keepdims=True))
    prob_round = attn_prob.astype(jnp.bfloat16).astype(jnp.float32)
    context = jnp.einsum('chmn,cnhd->cmhd', prob_round, value_heads).astype(jnp.bfloat16)
    grad_heads = ctx_grad.reshape(CH_DEV, SPAN, HEADS, HEAD_DIM).astype(jnp.float32)
    value_grad = jnp.einsum('chmn,cmhd->cnhd', prob_round, grad_heads).astype(jnp.bfloat16)
    prob_grad = jnp.einsum('cmhd,cnhd->chmn', grad_heads, value_heads)
    score_grad = attn_prob * (prob_grad - lax.optimization_barrier(jnp.sum(attn_prob * prob_grad, axis=-1, keepdims=True)))
    score_grad = score_grad.astype(jnp.bfloat16).astype(jnp.float32)
    query_grad = (jnp.einsum('chmn,cnhd->cmhd', score_grad, key_heads) * softmax_scale).astype(jnp.bfloat16)
    key_grad = jnp.einsum('chmn,cmhd->cnhd', score_grad, query_heads).astype(jnp.bfloat16)
    query_grad = query_grad.reshape(CH_DEV * SPAN, INNER)
    key_grad = key_grad.reshape(CH_DEV * NBR * NT, INNER)
    value_grad = value_grad.reshape(CH_DEV * NBR * NT, INNER)
    grad_query = jnp.dot(normed.T, query_grad, preferred_element_type=jnp.float32)
    grad_key = jnp.dot(latent_rows.T, key_grad, preferred_element_type=jnp.float32)
    grad_value = jnp.dot(latent_rows.T, value_grad, preferred_element_type=jnp.float32)
    return (context.reshape(CH_DEV * SPAN, INNER), grad_query, grad_key, grad_value)

def reference(tokens, ctx_cotangent, latent_cache, nbr_ids, w_query, w_key, w_value):
    blocks = N_DP * N_SHARD
    token_blocks = tokens.reshape(blocks, CH_DEV * SPAN, D)
    grad_blocks = ctx_cotangent.reshape(blocks, CH_DEV * SPAN, INNER)
    id_blocks = nbr_ids.reshape(blocks, CH_DEV * NBR)

    def one_block(sums, pieces):
        token_rows, grad_rows, id_rows = pieces
        as_float = token_rows.astype(jnp.float32)
        normed = (as_float * lax.rsqrt(lax.optimization_barrier(jnp.mean(as_float * as_float, axis=-1, keepdims=True)) + 1e-06)).astype(jnp.bfloat16)
        latent_rows = latent_cache[id_rows.astype(jnp.int32)].reshape(CH_DEV * NBR * NT, LAT)
        context, grad_query, grad_key, grad_value = attend_block(normed, latent_rows, grad_rows, w_query, w_key, w_value)
        return ((sums[0] + grad_query, sums[1] + grad_key, sums[2] + grad_value), context)
    start_sums = (jnp.zeros((D, INNER), jnp.float32), jnp.zeros((LAT, INNER), jnp.float32), jnp.zeros((LAT, INNER), jnp.float32))
    sums, contexts = lax.scan(one_block, start_sums, (token_blocks, grad_blocks, id_blocks))
    return (contexts.reshape(TOKENS, INNER), sums[0], sums[1], sums[2])
```

```python
import functools

import jax
import jax.numpy as jnp
from jax import lax
from jax.experimental import pallas as pl
from jax.experimental.pallas import tpu as pltpu
from jax.sharding import PartitionSpec as P

LAT = 896
HEADS = 8
HEAD_DIM = 128
SPAN = 64
NBR = 2
NT = 128
CH_DEV = 4
INNER = 1024
D = 2048
CHIPS = 64
PARTS = ((0, 384), (384, 384), (768, 256))
WIDTHS = tuple(w for _, w in PARTS) * 2
LEVELS = 6
OFFSETS = (0, 32, 48, 56, 60, 62)
NT_DIMS = (((1,), (1,)), ((), ()))
MESH = pl.DeviceIdType.MESH


def nt_dot(a, b):
    return lax.dot_general(a, b, NT_DIMS, preferred_element_type=jnp.float32)


def nn_dot(a, b):
    return jnp.dot(a, b, preferred_element_type=jnp.float32)


def place(chip, part):
    code = chip ^ ((chip >> 1) & 21)
    return ((code << part) | (code >> (LEVELS - part))) & (CHIPS - 1)


def one_hot(rows, columns, wanted):
    r = lax.broadcasted_iota(jnp.int32, (rows, columns), 0)
    c = lax.broadcasted_iota(jnp.int32, (rows, columns), 1)
    return wanted(r, c).astype(jnp.float32).astype(jnp.bfloat16)


def compute_kernel(
    tok, cot, lat, wq, wk, wv, ctx, x0, x1, x2, x3, x4, x5, normed, q, kb, vb, qg, kg, vg, lat_t
):
    scale = HEAD_DIM ** (-0.5)
    outs = (x0, x1, x2, x3, x4, x5)

    @pl.loop(0, 8)
    def _(i):
        rows = pl.ds(pl.multiple_of(i * 32, 32), 32)
        t = tok[rows, :].astype(jnp.float32)
        inverse = lax.rsqrt(jnp.mean(t * t, axis=-1, keepdims=True) + 1e-06)
        normed[rows, :] = (t * inverse).astype(jnp.bfloat16)

    @pl.loop(0, 4)
    def _(i):
        cols = pl.ds(pl.multiple_of(i * 256, 256), 256)
        q[:, cols] = (nn_dot(normed[...], wq[:, cols]) * scale).astype(jnp.bfloat16)

    eye = one_hot(128, 128, lambda r, c: r == c)
    zero = jnp.zeros((SPAN, HEAD_DIM), jnp.bfloat16)

    def diagonal(ref, rows, at):
        a = ref[rows, at : at + HEAD_DIM]
        b = ref[rows, at + HEAD_DIM : at + 2 * HEAD_DIM]
        return jnp.concatenate(
            [jnp.concatenate([a, zero], axis=1), jnp.concatenate([zero, b], axis=1)], axis=0
        )

    @pl.loop(0, CH_DEV)
    def _(c):
        rows = pl.ds(pl.multiple_of(c * 256, 256), 256)
        trows = pl.ds(pl.multiple_of(c * SPAN, SPAN), SPAN)
        block = lat[rows, :]
        for at in range(0, INNER, 256):
            kb[:, at : at + 256] = nn_dot(block, wk[:, at : at + 256]).astype(jnp.bfloat16)
            vb[:, at : at + 256] = nn_dot(block, wv[:, at : at + 256]).astype(jnp.bfloat16)
        for at in range(0, INNER, 256):
            mid = at + HEAD_DIM
            end = at + 256
            kp = kb[:, at:end]
            vp = vb[:, at:end]
            q2 = diagonal(q, trows, at)
            g2 = diagonal(cot, trows, at)
            scores = nt_dot(kp, q2)
            e = jnp.exp(scores - jnp.max(scores, axis=0, keepdims=True))
            prob = e * (1.0 / jnp.sum(e, axis=0, keepdims=True))
            prob_t = prob.astype(jnp.bfloat16)
            prob_r = nt_dot(eye, prob_t).astype(jnp.bfloat16)
            c2 = nn_dot(prob_r, vp).astype(jnp.bfloat16)
            ctx[trows, at:mid] = c2[:SPAN, :HEAD_DIM]
            ctx[trows, mid:end] = c2[SPAN:, HEAD_DIM:]
            vg[rows, at:end] = nn_dot(prob_t, g2).astype(jnp.bfloat16)
            pg = nt_dot(vp, g2)
            sg_t = (prob * (pg - jnp.sum(prob * pg, axis=0, keepdims=True))).astype(jnp.bfloat16)
            kg[rows, at:end] = nn_dot(sg_t, q2).astype(jnp.bfloat16)
            sg = nt_dot(eye, sg_t).astype(jnp.bfloat16)
            qg2 = (nn_dot(sg, kp) * scale).astype(jnp.bfloat16)
            qg[trows, at:mid] = qg2[:SPAN, :HEAD_DIM]
            qg[trows, mid:end] = qg2[SPAN:, HEAD_DIM:]

    eye_wide = one_hot(256, 256, lambda r, c: r == c)

    @pl.loop(0, 8)
    def _(i):
        cols = pl.ds(pl.multiple_of(i * 256, 256), 256)
        turned = nt_dot(eye_wide, normed[:, cols]).astype(jnp.bfloat16)
        for p, (at, width) in enumerate(PARTS):
            r = nn_dot(turned, qg[:, at : at + width]).astype(jnp.bfloat16)
            for j in range(16):
                outs[p][j & 1, place(8 * i + (j >> 1), p)] = r[16 * j : 16 * j + 16, :]

    for b, (at, width) in enumerate(((0, 256), (128, 384), (384, 384), (640, 256))):
        pick = one_hot(
            256,
            width,
            lambda r, c: (c + at == 224 * b + 7 * (r >> 3) + (r & 7)) & ((r & 7) < 7),
        )
        for rat in range(0, 1024, 256):
            lat_t[256 * b : 256 * b + 256, rat : rat + 256] = nt_dot(
                pick, lat[rat : rat + 256, at : at + width]
            ).astype(jnp.bfloat16)

    @pl.loop(0, 4)
    def _(b):
        rows = pl.ds(pl.multiple_of(b * 256, 256), 256)
        turned = lat_t[rows, :]
        for p, (at, width) in enumerate(PARTS):
            rk = nn_dot(turned, kg[:, at : at + width])
            rv = nn_dot(turned, vg[:, at : at + width])
            for j in range(32):
                both = jnp.concatenate([rk[8 * j : 8 * j + 8], rv[8 * j : 8 * j + 8]], axis=0)
                outs[3 + p][j & 1, place(16 * b + (j >> 1), 3 + p)] = both.astype(jnp.bfloat16)


def compute(tok, cot, lat, wq, wk, wv):
    bf = jnp.bfloat16
    vmem = pl.BlockSpec(memory_space=pltpu.VMEM)
    return pl.pallas_call(
        compute_kernel,
        out_shape=(
            jax.ShapeDtypeStruct((256, INNER), bf),
            *(jax.ShapeDtypeStruct((2, CHIPS, 16, w), bf) for w in WIDTHS),
        ),
        in_specs=[vmem] * 6,
        out_specs=(vmem,) * 7,
        scratch_shapes=[
            pltpu.VMEM((256, D), bf),
            pltpu.VMEM((256, INNER), bf),
            pltpu.VMEM((256, INNER), bf),
            pltpu.VMEM((256, INNER), bf),
            pltpu.VMEM((256, INNER), bf),
            pltpu.VMEM((1024, INNER), bf),
            pltpu.VMEM((1024, INNER), bf),
            pltpu.VMEM((1024, 1024), bf),
        ],
        compiler_params=pltpu.CompilerParams(vmem_limit_bytes=48 * 1024 * 1024),
        name="attend",
    )(tok, cot, lat, wq, wk, wv)


def flip(coordinate, high):
    return 3 - coordinate if high else coordinate ^ 1


def reduce_kernel(*refs):
    xs, (gq, gk, gv) = refs[:6], refs[6:9]
    crecv, acc, snd, rcv = refs[9:15], refs[15:21], refs[21:27], refs[27:33]
    csem, send_sem, recv_sem = refs[33:]
    dp = lax.axis_index("dp")
    shard = lax.axis_index("shard")
    z, x, y, core = dp // 4, dp % 4, shard // 2, shard % 2
    other = (dp, y * 2 + (1 - core))
    partners = []
    for d in range(LEVELS):
        high = d % 2 == 0
        if d < 2:
            partners.append((flip(z, high) * 4 + x, shard))
        elif d < 4:
            partners.append((z * 4 + flip(x, high), shard))
        else:
            partners.append((dp, flip(y, high) * 2 + core))
    mine = place(z * 16 + x * 4 + y, 0)

    barrier = pltpu.get_barrier_semaphore()
    for device in [other] + partners:
        pl.semaphore_signal(barrier, inc=1, device_id=device, device_id_type=MESH)
    pl.semaphore_wait(barrier, 7)

    pending = []
    first = []
    for p in range(6):
        copy = pltpu.make_async_remote_copy(
            src_ref=xs[p].at[1 - core],
            dst_ref=crecv[p],
            send_sem=csem.at[0, p],
            recv_sem=csem.at[1, p],
            device_id=other,
            device_id_type=MESH,
        )
        copy.start()
        first.append(copy)
        pending.append(copy)
    coming = first
    base = [0] * 6
    for k in range(LEVELS):
        half = CHIPS >> (k + 1)
        step = min(half, 8)
        started = []
        for p in range(6):
            d = (p + k) % LEVELS
            bit = (mine >> (LEVELS - 1 - d)) & 1
            away = base[p] + (1 - bit) * half
            keep = base[p] + bit * half
            coming[p].wait_recv()

            def summed(at, p=p, k=k, step=step):
                where = pl.ds(at, step)
                if k == 0:
                    return xs[p][core, where].astype(jnp.float32) + crecv[p][where].astype(
                        jnp.float32
                    )
                back = pl.ds(OFFSETS[k - 1] + at - base[p], step)
                return acc[p][where] + rcv[p][back].astype(jnp.float32)

            @pl.loop(0, half // step)
            def _(i, p=p, k=k, away=away, step=step, summed=summed):
                snd[p][pl.ds(OFFSETS[k] + i * step, step)] = summed(away + i * step).astype(
                    jnp.bfloat16
                )

            copy = pltpu.make_async_remote_copy(
                src_ref=snd[p].at[pl.ds(OFFSETS[k], half)],
                dst_ref=rcv[p].at[pl.ds(OFFSETS[k], half)],
                send_sem=send_sem.at[k, p],
                recv_sem=recv_sem.at[k, p],
                device_id=partners[d],
                device_id_type=MESH,
            )
            copy.start()
            started.append(copy)
            pending.append(copy)

            @pl.loop(0, half // step)
            def _(i, p=p, keep=keep, step=step, summed=summed):
                acc[p][pl.ds(keep + i * step, step)] = summed(keep + i * step)

            base[p] = keep
        coming = started
    for p in range(6):
        coming[p].wait_recv()
        total = acc[p][base[p]] + rcv[p][OFFSETS[5]].astype(jnp.float32)
        at, width = PARTS[p % 3]
        if p < 3:
            gq[:, at : at + width] = total
        else:
            gk[:, at : at + width] = total[0:7]
            gv[:, at : at + width] = total[8:15]
    for copy in pending:
        copy.wait_send()


def reduce_scatter(xs):
    vmem = pl.BlockSpec(memory_space=pltpu.VMEM)
    f32, bf = jnp.float32, jnp.bfloat16
    return pl.pallas_call(
        reduce_kernel,
        out_shape=(
            jax.ShapeDtypeStruct((16, INNER), f32),
            jax.ShapeDtypeStruct((7, INNER), f32),
            jax.ShapeDtypeStruct((7, INNER), f32),
        ),
        in_specs=[vmem] * 6,
        out_specs=(vmem,) * 3,
        scratch_shapes=[
            *(pltpu.VMEM((CHIPS, 16, w), bf) for w in WIDTHS),
            *(pltpu.VMEM((CHIPS, 16, w), f32) for w in WIDTHS),
            *(pltpu.VMEM((CHIPS, 16, w), bf) for w in WIDTHS),
            *(pltpu.VMEM((CHIPS, 16, w), bf) for w in WIDTHS),
            pltpu.SemaphoreType.DMA((2, 6)),
            pltpu.SemaphoreType.DMA((LEVELS, 6)),
            pltpu.SemaphoreType.DMA((LEVELS, 6)),
        ],
        compiler_params=pltpu.CompilerParams(
            collective_id=1, has_side_effects=True, vmem_limit_bytes=40 * 1024 * 1024
        ),
        name="reduce_halving",
    )(*xs)


def copy_for_each(array, axis):
    count = lax.axis_size(axis)
    return lax.all_to_all(
        jnp.broadcast_to(array[None], (count, *array.shape)), axis, 0, 0, tiled=True
    )


def laid_out(parts, dim):
    parts = jnp.moveaxis(parts, 0, dim)
    dims = parts.shape
    return parts.reshape(*dims[:dim], dims[dim] * dims[dim + 1], *dims[dim + 2 :])


def collect(array, axis, dim):
    parts = copy_for_each(array, axis)
    return laid_out(parts, dim)


def sent_together(arrays, axis, dim, along):
    both = jnp.concatenate(arrays, axis=along)
    whole, at, gathered = (lax.all_gather(both, axis, axis=dim, tiled=True), 0, [])
    for a in arrays:
        gathered.append(lax.slice_in_dim(whole, at, at + a.shape[along], axis=along))
        at += a.shape[along]
    return tuple(gathered)


def body(tokens, ctx_cotangent, latent_cache, nbr_ids, w_query, w_key, w_value):
    owner_count = lax.axis_size("dp")
    shard_count = lax.axis_size("shard")
    owner_rows = latent_cache.shape[0]
    slice_tokens = latent_cache.shape[1]
    requests = nbr_ids.reshape(-1)
    gathered = collect(requests, "shard", 0)
    slot_count = 2 * gathered.shape[0] // owner_count
    owner_of = gathered // owner_rows
    within_row = gathered % owner_rows
    onehot = (owner_of[:, None] == jnp.arange(owner_count, dtype=jnp.int32)[None, :]).astype(
        jnp.int32
    )
    earlier = jnp.cumsum(onehot, axis=0) - onehot
    position = jnp.sum(earlier * onehot, axis=1)
    slot_of = owner_of * slot_count + position
    outgoing = jnp.zeros((owner_count * slot_count,), jnp.int32).at[slot_of].set(within_row)
    outgoing = outgoing.reshape(owner_count, slot_count)
    asked_rows = lax.all_to_all(outgoing, "dp", split_axis=0, concat_axis=0, tiled=True)
    fetched = latent_cache[asked_rows.reshape(-1)]
    fetched = fetched.reshape(asked_rows.shape[0], asked_rows.shape[1], slice_tokens, LAT)
    replies = lax.all_to_all(fetched, "dp", split_axis=0, concat_axis=0, tiled=True)
    arrived = replies.reshape(owner_count * slot_count, slice_tokens, LAT)
    chosen = arrived[slot_of].reshape(shard_count, -1, slice_tokens, LAT)
    latents = lax.all_to_all(chosen, "shard", split_axis=0, concat_axis=2, tiled=True)
    latent_rows = latents.reshape(-1, LAT)
    pieces = sent_together((w_key, w_value), "shard", 0, 1)
    whole_query = lax.all_gather(w_query, "shard", axis=0, tiled=True)
    context, *partial = compute(tokens, ctx_cotangent, latent_rows, whole_query, *pieces)
    return (context, *reduce_scatter(partial))


def solution(mesh):
    return jax.shard_map(
        body,
        mesh=mesh,
        in_specs=(
            P(("dp", "shard"), None),
            P(("dp", "shard"), None),
            P("dp", "shard", None),
            P(("dp", "shard"), None),
            P("shard", None),
            P("shard", None),
            P("shard", None),
        ),
        out_specs=(
            P(("dp", "shard"), None),
            P(("dp", "shard"), None),
            P(("dp", "shard"), None),
            P(("dp", "shard"), None),
        ),
        check_vma=False,
    )
```

```python
import functools

import jax
import jax.numpy as jnp
from jax import lax
from jax.experimental import pallas as pl
from jax.experimental.pallas import tpu as pltpu
from jax.sharding import PartitionSpec as P

LAT = 896
HEADS = 8
HEAD_DIM = 128
SPAN = 64
NBR = 2
NT = 128
CH_DEV = 4
INNER = 1024
D = 2048
CHIPS = 64
PARTS = ((0, 384), (384, 384), (768, 256))
WIDTHS = tuple(w for _, w in PARTS) * 2
LEVELS = 6
CHUNKS = ((0, 384), (384, 256), (640, 256))
DP_ORDER = (1, 4, 3, 12, 2, 8, 5, 15, 7, 13, 6, 9, 11, 14, 10)
WEIGHT_ROWS = (256, 112, 112)
WEIGHT_CUTS = (128, 64, 48)
OFFSETS = (0, 32, 48, 56, 60, 62)
NT_DIMS = (((1,), (1,)), ((), ()))
MESH = pl.DeviceIdType.MESH


def nt_dot(a, b):
    return lax.dot_general(a, b, NT_DIMS, preferred_element_type=jnp.float32)


def nn_dot(a, b):
    return jnp.dot(a, b, preferred_element_type=jnp.float32)


def place(chip, part):
    code = chip ^ ((chip >> 1) & 21)
    return ((code << part) | (code >> (LEVELS - part))) & (CHIPS - 1)


def one_hot(rows, columns, wanted):
    r = lax.broadcasted_iota(jnp.int32, (rows, columns), 0)
    c = lax.broadcasted_iota(jnp.int32, (rows, columns), 1)
    return wanted(r, c).astype(jnp.float32).astype(jnp.bfloat16)


def running_count(mask, lane):
    for s in (1, 2, 4, 8, 16, 32):
        mask = mask + jnp.where(lane >= s, pltpu.roll(mask, s, 1), 0)
    return mask


def packed_left(mask, values, lane):
    shift = jnp.where(mask > 0, lane - running_count(mask, lane) + 1, 0)
    values = jnp.where(mask > 0, values, 0)
    for b in (1, 2, 4, 8, 16, 32):
        moves = (shift & b) > 0
        values = jnp.where(moves, 0, values) + pltpu.roll(jnp.where(moves, values, 0), 128 - b, 1)
        shift = jnp.where(moves, 0, shift) + pltpu.roll(jnp.where(moves, shift, 0), 128 - b, 1)
    return values


def flip(coordinate, high):
    return 3 - coordinate if high else coordinate ^ 1


def whole_kernel(
    id_row, tok_in, cot_in, cache_in, wq_in, wk_in, wv_in, ctx, gq, gk, gv, *scratch
):
    it = iter(scratch)

    def take(n=None):
        return next(it) if n is None else tuple(next(it) for _ in range(n))

    ids_shard, id_group, ids_dp, asked_v, slots_v, asked_s, slots_s = take(7)
    cache, tok, cot = take(3)
    weights = take(3)
    wq, wk, wv = weights
    outgoing, replies, chosen = take(3), take(3), take(3)
    lat = take()
    normed, q, kb, vb, qg, kg, vg, lat_t = take(8)
    xs, crecv, acc, snd, rcv = take(6), take(6), take(6), take(6), take(6)
    local_sem, id_send, id_recv, gid_send, gid_recv, w_send, w_recv = take(7)
    dp_send, dp_recv, sh_send, sh_recv, csem, send_sem, recv_sem = take(7)

    dp = lax.axis_index("dp")
    shard = lax.axis_index("shard")
    z, x, y, core = dp // 4, dp % 4, shard // 2, shard % 2
    other = (dp, y * 2 + (1 - core))
    pending = []

    def send(src, dst, ss, rs, device):
        copy = pltpu.make_async_remote_copy(
            src_ref=src,
            dst_ref=dst,
            send_sem=ss,
            recv_sem=rs,
            device_id=device,
            device_id_type=MESH,
        )
        copy.start()
        pending.append(copy)
        return copy

    barrier = pltpu.get_barrier_semaphore()
    for r in range(1, 8):
        pl.semaphore_signal(barrier, inc=1, device_id=(dp, shard ^ r), device_id_type=MESH)
    for r in DP_ORDER:
        pl.semaphore_signal(barrier, inc=1, device_id=(dp ^ r, shard), device_id_type=MESH)

    def w_rows(a, row, side, start=0, size=None):
        n = WEIGHT_ROWS[a]
        at = pl.multiple_of((row * 2 + side) * n + start, 16)
        return weights[a].at[pl.ds(at, n if size is None else size)]

    own_weights = []
    for a, src in enumerate((wq_in, wk_in, wv_in)):
        copy = pltpu.make_async_copy(src, w_rows(a, y, core), local_sem.at[a])
        copy.start()
        own_weights.append(copy)
    loads = []
    for n, (src, dst) in enumerate(((cache_in, cache), (tok_in, tok), (cot_in, cot))):
        copy = pltpu.make_async_copy(src, dst, local_sem.at[3 + n])
        copy.start()
        loads.append(copy)

    pl.semaphore_wait(barrier, 22)

    ids_shard[shard] = id_row[...]
    asks = [
        send(id_row, ids_shard.at[shard], id_send.at[r], id_recv.at[r], (dp, shard ^ r))
        for r in range(1, 8)
    ]
    for copy in asks:
        copy.wait_recv()
    group = ids_shard[0]
    for s in range(1, 8):
        group = group + ids_shard[s]
    id_group[...] = group
    ids_dp[dp] = group
    asks = [
        send(id_group, ids_dp.at[dp], gid_send.at[r], gid_recv.at[r], (dp ^ r, shard))
        for r in DP_ORDER
    ]

    up, down, far = (y + 1) % 4, (y + 3) % 4, (y + 2) % 4
    for copy in own_weights:
        copy.wait()
    kinds = {}

    def send_weights(kind, row, device, part=None):
        copies = []
        for a in range(3):
            n, cut = WEIGHT_ROWS[a], WEIGHT_CUTS[a]
            start, size = ((0, n), (0, cut), (cut, n - cut))[0 if part is None else 1 + part]
            ref = w_rows(a, row, core, start, size)
            copies.append(send(ref, ref, w_send.at[kind, a], w_recv.at[kind, a], device))
        kinds[kind] = copies

    def arrived(kind):
        for copy in kinds[kind]:
            copy.wait_recv()

    send_weights(0, y, (dp, up * 2 + core))
    send_weights(1, y, (dp, down * 2 + core))
    send_weights(2, y, other)

    lane = lax.broadcasted_iota(jnp.int32, (16, 128), 1)
    owners = lax.broadcasted_iota(jnp.int32, (16, 128), 0)
    mine = jnp.where((lane < 64) & ((group[0:1] >> 7) == owners), 1, 0)
    places = jnp.where(mine > 0, owners * 8 + running_count(mine, lane) - 1, 0)
    slots = places[0:1]
    for o in range(1, 16):
        slots = slots + places[o : o + 1]
    slots_v[...] = jnp.broadcast_to(slots, (8, 128))

    for copy in asks:
        copy.wait_recv()
    ids = jnp.concatenate([ids_dp[g][0:1] for g in range(16)], axis=0)
    wanted = jnp.where((lane < 64) & ((ids >> 7) == dp), 1, 0)
    asked_v[...] = packed_left(wanted, ids & 127, lane)
    to_scalar = [
        pltpu.make_async_copy(asked_v, asked_s, local_sem.at[6]),
        pltpu.make_async_copy(slots_v, slots_s, local_sem.at[7]),
    ]
    for copy in to_scalar:
        copy.start()
    loads[0].wait()
    for copy in to_scalar:
        copy.wait()

    @pl.loop(0, 16)
    def _(g):
        for j in range(8):
            row = asked_s[g, j]
            for c, (at, width) in enumerate(CHUNKS):
                outgoing[c][g, j] = cache[row, :, at : at + width]

    fetches = []
    for c in range(3):
        own = pl.ds(pl.multiple_of(dp * 8, 8), 8)
        fetches.append(
            [
                send(
                    outgoing[c].at[dp ^ r],
                    replies[c].at[own],
                    dp_send.at[c, r],
                    dp_recv.at[c, r],
                    (dp ^ r, shard),
                )
                for r in DP_ORDER
            ]
        )
    for c in range(3):
        replies[c][pl.ds(pl.multiple_of(dp * 8, 8), 8)] = outgoing[c][dp]

    loads[1].wait()
    loads[2].wait()

    @pl.loop(0, 8)
    def _(i):
        rows = pl.ds(pl.multiple_of(i * 32, 32), 32)
        t = tok[rows, :].astype(jnp.float32)
        inverse = lax.rsqrt(jnp.mean(t * t, axis=-1, keepdims=True) + 1e-06)
        normed[rows, :] = (t * inverse).astype(jnp.bfloat16)

    spread = []

    def hand_on(c):
        at, width = CHUNKS[c]
        for copy in fetches[c]:
            copy.wait_recv()

        @pl.loop(0, 8)
        def _(s):
            for i in range(8):
                chosen[c][s, i] = replies[c][slots_s[0, s * 8 + i]]

        for r in range(1, 8):
            spread.append(
                send(
                    chosen[c].at[shard ^ r],
                    lat.at[:, shard, :, pl.ds(at, width)],
                    sh_send.at[c, r],
                    sh_recv.at[c, r],
                    (dp, shard ^ r),
                )
            )
        lat[:, shard, :, at : at + width] = chosen[c][shard]

    arrived(0)
    send_weights(3, down, (dp, up * 2 + core), 0)
    send_weights(5, down, other)
    arrived(1)
    send_weights(4, up, (dp, down * 2 + core), 1)
    send_weights(6, up, other)
    hand_on(0)
    arrived(3)
    send_weights(7, far, other, 0)
    arrived(4)
    send_weights(8, far, other, 1)
    hand_on(1)
    for kind in (2, 5, 6, 7, 8):
        arrived(kind)

    scale = HEAD_DIM ** (-0.5)

    @pl.loop(0, 4)
    def _(i):
        cols = pl.ds(pl.multiple_of(i * 256, 256), 256)
        q[:, cols] = (nn_dot(normed[...], wq[:, cols]) * scale).astype(jnp.bfloat16)

    hand_on(2)
    for copy in spread:
        copy.wait_recv()

    eye = one_hot(128, 128, lambda r, c: r == c)
    zero = jnp.zeros((SPAN, HEAD_DIM), jnp.bfloat16)

    def diagonal(ref, rows, at):
        a = ref[rows, at : at + HEAD_DIM]
        b = ref[rows, at + HEAD_DIM : at + 2 * HEAD_DIM]
        return jnp.concatenate(
            [jnp.concatenate([a, zero], axis=1), jnp.concatenate([zero, b], axis=1)], axis=0
        )

    @pl.loop(0, CH_DEV)
    def _(c):
        rows = pl.ds(pl.multiple_of(c * 256, 256), 256)
        trows = pl.ds(pl.multiple_of(c * SPAN, SPAN), SPAN)
        block = lat[pl.ds(2 * c, 2)].reshape(256, LAT)
        for at in range(0, INNER, 256):
            kb[:, at : at + 256] = nn_dot(block, wk[:, at : at + 256]).astype(jnp.bfloat16)
            vb[:, at : at + 256] = nn_dot(block, wv[:, at : at + 256]).astype(jnp.bfloat16)
        for at in range(0, INNER, 256):
            mid = at + HEAD_DIM
            end = at + 256
            kp = kb[:, at:end]
            vp = vb[:, at:end]
            q2 = diagonal(q, trows, at)
            g2 = diagonal(cot, trows, at)
            scores = nt_dot(kp, q2)
            e = jnp.exp(scores - jnp.max(scores, axis=0, keepdims=True))
            prob = e * (1.0 / jnp.sum(e, axis=0, keepdims=True))
            prob_t = prob.astype(jnp.bfloat16)
            prob_r = nt_dot(eye, prob_t).astype(jnp.bfloat16)
            c2 = nn_dot(prob_r, vp).astype(jnp.bfloat16)
            ctx[trows, at:mid] = c2[:SPAN, :HEAD_DIM]
            ctx[trows, mid:end] = c2[SPAN:, HEAD_DIM:]
            vg[rows, at:end] = nn_dot(prob_t, g2).astype(jnp.bfloat16)
            pg = nt_dot(vp, g2)
            sg_t = (prob * (pg - jnp.sum(prob * pg, axis=0, keepdims=True))).astype(jnp.bfloat16)
            kg[rows, at:end] = nn_dot(sg_t, q2).astype(jnp.bfloat16)
            sg = nt_dot(eye, sg_t).astype(jnp.bfloat16)
            qg2 = (nn_dot(sg, kp) * scale).astype(jnp.bfloat16)
            qg[trows, at:mid] = qg2[:SPAN, :HEAD_DIM]
            qg[trows, mid:end] = qg2[SPAN:, HEAD_DIM:]

    partners = []
    for d in range(LEVELS):
        high = d % 2 == 0
        if d < 2:
            partners.append((flip(z, high) * 4 + x, shard))
        elif d < 4:
            partners.append((z * 4 + flip(x, high), shard))
        else:
            partners.append((dp, flip(y, high) * 2 + core))
    here = place(z * 16 + x * 4 + y, 0)
    coming = [None] * 6
    base = [0] * 6
    root = [0] * 6

    def to_other_core(p):
        coming[p] = send(xs[p].at[1 - core], crecv[p], csem.at[0, p], csem.at[1, p], other)

    def halve(k, p):
        half = CHIPS >> (k + 1)
        step = min(half, 8)
        d = (p + k) % LEVELS
        bit = (here >> (LEVELS - 1 - d)) & 1
        away = base[p] + (1 - bit) * half
        keep = base[p] + bit * half
        coming[p].wait_recv()
        if k == 0:
            root[p] = keep

        def summed(at):
            where = pl.ds(at, step)
            if k == 0:
                return xs[p][core, where].astype(jnp.float32) + crecv[p][where].astype(jnp.float32)
            back = pl.ds(OFFSETS[k - 1] + at - base[p], step)
            return acc[p][pl.ds(at - root[p], step)] + rcv[p][back].astype(jnp.float32)

        @pl.loop(0, half // step)
        def _(i):
            snd[p][pl.ds(OFFSETS[k] + i * step, step)] = summed(away + i * step).astype(
                jnp.bfloat16
            )

        span = pl.ds(OFFSETS[k], half)
        copy = send(
            snd[p].at[span], rcv[p].at[span], send_sem.at[k, p], recv_sem.at[k, p], partners[d]
        )

        @pl.loop(0, half // step)
        def _(i):
            acc[p][pl.ds(keep - root[p] + i * step, step)] = summed(keep + i * step)

        base[p] = keep
        coming[p] = copy

    eye_wide = one_hot(256, 256, lambda r, c: r == c)

    @pl.loop(0, 8)
    def _(i):
        cols = pl.ds(pl.multiple_of(i * 256, 256), 256)
        turned = nt_dot(eye_wide, normed[:, cols]).astype(jnp.bfloat16)
        for p, (at, width) in enumerate(PARTS):
            r = nn_dot(turned, qg[:, at : at + width]).astype(jnp.bfloat16)
            for j in range(16):
                xs[p][j & 1, place(8 * i + (j >> 1), p)] = r[16 * j : 16 * j + 16, :]

    for p in range(3):
        to_other_core(p)

    for b, (at, width) in enumerate(((0, 256), (128, 384), (384, 384), (640, 256))):
        pick = one_hot(
            256,
            width,
            lambda r, c: (c + at == 224 * b + 7 * (r >> 3) + (r & 7)) & ((r & 7) < 7),
        )
        for n in range(4):
            block = lat[2 * n : 2 * n + 2, :, :, at : at + width].reshape(256, width)
            lat_t[256 * b : 256 * b + 256, 256 * n : 256 * n + 256] = nt_dot(pick, block).astype(
                jnp.bfloat16
            )

    for p in range(3):
        halve(0, p)

    for p, (at, width) in enumerate(PARTS):

        @pl.loop(0, 4)
        def _(b):
            turned = lat_t[pl.ds(pl.multiple_of(b * 256, 256), 256), :]
            rk = nn_dot(turned, kg[:, at : at + width])
            rv = nn_dot(turned, vg[:, at : at + width])
            for j in range(32):
                both = jnp.concatenate([rk[8 * j : 8 * j + 8], rv[8 * j : 8 * j + 8]], axis=0)
                xs[3 + p][j & 1, place(16 * b + (j >> 1), 3 + p)] = both.astype(jnp.bfloat16)

        to_other_core(3 + p)

    for p in range(3, 6):
        halve(0, p)
    for k in range(1, LEVELS):
        for p in range(6):
            halve(k, p)
    for p in range(6):
        coming[p].wait_recv()
        total = acc[p][base[p] - root[p]] + rcv[p][OFFSETS[5]].astype(jnp.float32)
        at, width = PARTS[p % 3]
        if p < 3:
            gq[:, at : at + width] = total
        else:
            gk[:, at : at + width] = total[0:7]
            gv[:, at : at + width] = total[8:15]
    for copy in pending:
        copy.wait_send()


def body(tokens, ctx_cotangent, latent_cache, nbr_ids, w_query, w_key, w_value):
    lane = jnp.arange(128, dtype=jnp.int32)
    id_row = jnp.where(
        lane // 8 == lax.axis_index("shard"), jnp.tile(nbr_ids.reshape(-1), 16), 0
    )
    id_row = jnp.broadcast_to(id_row[None], (8, 128))
    f32, bf, i32 = jnp.float32, jnp.bfloat16, jnp.int32
    vmem = pl.BlockSpec(memory_space=pltpu.VMEM)
    hbm = pl.BlockSpec(memory_space=pl.ANY)
    dma = pltpu.SemaphoreType.DMA
    widths = [w for _, w in CHUNKS]
    return pl.pallas_call(
        whole_kernel,
        out_shape=(
            jax.ShapeDtypeStruct((256, INNER), bf),
            jax.ShapeDtypeStruct((16, INNER), f32),
            jax.ShapeDtypeStruct((7, INNER), f32),
            jax.ShapeDtypeStruct((7, INNER), f32),
        ),
        in_specs=[vmem] + [hbm] * 6,
        out_specs=(vmem,) * 4,
        scratch_shapes=[
            pltpu.VMEM((8, 8, 128), i32),
            pltpu.VMEM((8, 128), i32),
            pltpu.VMEM((16, 8, 128), i32),
            pltpu.VMEM((16, 128), i32),
            pltpu.VMEM((8, 128), i32),
            pltpu.SMEM((16, 128), i32),
            pltpu.SMEM((8, 128), i32),
            pltpu.VMEM((128, 16, LAT), bf),
            pltpu.VMEM((256, D), bf),
            pltpu.VMEM((256, INNER), bf),
            pltpu.VMEM((D, INNER), bf),
            pltpu.VMEM((LAT, INNER), bf),
            pltpu.VMEM((LAT, INNER), bf),
            *(pltpu.VMEM((16, 8, 16, w), bf) for w in widths),
            *(pltpu.VMEM((128, 16, w), bf) for w in widths),
            *(pltpu.VMEM((8, 8, 16, w), bf) for w in widths),
            pltpu.VMEM((8, 8, 16, LAT), bf),
            pltpu.VMEM((256, D), bf),
            pltpu.VMEM((256, INNER), bf),
            pltpu.VMEM((256, INNER), bf),
            pltpu.VMEM((256, INNER), bf),
            pltpu.VMEM((256, INNER), bf),
            pltpu.VMEM((1024, INNER), bf),
            pltpu.VMEM((1024, INNER), bf),
            pltpu.VMEM((1024, 1024), bf),
            *(pltpu.VMEM((2, CHIPS, 16, w), bf) for w in WIDTHS),
            *(pltpu.VMEM((CHIPS, 16, w), bf) for w in WIDTHS),
            *(pltpu.VMEM((CHIPS // 2, 16, w), f32) for w in WIDTHS),
            *(pltpu.VMEM((CHIPS, 16, w), bf) for w in WIDTHS),
            *(pltpu.VMEM((CHIPS, 16, w), bf) for w in WIDTHS),
            dma((8,)),
            dma((8,)),
            dma((8,)),
            dma((16,)),
            dma((16,)),
            dma((9, 3)),
            dma((9, 3)),
            dma((3, 16)),
            dma((3, 16)),
            dma((3, 8)),
            dma((3, 8)),
            dma((2, 6)),
            dma((LEVELS, 6)),
            dma((LEVELS, 6)),
        ],
        compiler_params=pltpu.CompilerParams(
            collective_id=1, has_side_effects=True, vmem_limit_bytes=67043328
        ),
        name="retro",
    )(
        id_row,
        tokens,
        ctx_cotangent,
        latent_cache,
        w_query,
        w_key,
        w_value,
    )


def solution(mesh):
    return jax.shard_map(
        body,
        mesh=mesh,
        in_specs=(
            P(("dp", "shard"), None),
            P(("dp", "shard"), None),
            P("dp", "shard", None),
            P(("dp", "shard"), None),
            P("shard", None),
            P("shard", None),
            P("shard", None),
        ),
        out_specs=(
            P(("dp", "shard"), None),
            P(("dp", "shard"), None),
            P(("dp", "shard"), None),
            P(("dp", "shard"), None),
        ),
        check_vma=False,
    )
```

```python
import jax
import jax.numpy as jnp
from jax import lax
from jax.experimental import pallas as pl
from jax.experimental.pallas import tpu as pltpu
from jax.sharding import PartitionSpec as P

LAT = 896
HEADS = 8
HEAD_DIM = 128
SPAN = 64
NBR = 2
NT = 128
CH_DEV = 4
INNER = 1024
D = 2048
CHIPS = 64
LEVELS = 6
OFFSETS = (0, 32, 48)
TURNS = (0, 1, 2, 3, 4, 5, 0, 3, 0, 1, 2, 3, 4, 5, 1, 4)
CHUNKS = ((0, 384), (384, 384), (768, 128))
DP_ORDER = (1, 4, 3, 12, 2, 8, 5, 15, 7, 13, 6, 9, 11, 14, 10)
WEIGHT_ROWS = (256, 112, 112)
WEIGHT_CUTS = (128, 64, 48)
NT_DIMS = (((1,), (1,)), ((), ()))
MESH = pl.DeviceIdType.MESH


def nt_dot(a, b):
    return lax.dot_general(a, b, NT_DIMS, preferred_element_type=jnp.float32)


def nn_dot(a, b):
    return jnp.dot(a, b, preferred_element_type=jnp.float32)


def place(chip, part):
    code = chip ^ ((chip >> 1) & 21)
    return ((code << part) | (code >> (LEVELS - part))) & (CHIPS - 1)


def one_hot(rows, columns, wanted):
    r = lax.broadcasted_iota(jnp.int32, (rows, columns), 0)
    c = lax.broadcasted_iota(jnp.int32, (rows, columns), 1)
    return wanted(r, c).astype(jnp.float32).astype(jnp.bfloat16)


def running_count(mask, lane):
    for s in (1, 2, 4, 8, 16, 32):
        mask = mask + jnp.where(lane >= s, pltpu.roll(mask, s, 1), 0)
    return mask


def packed_left(mask, values, lane):
    shift = jnp.where(mask > 0, lane - running_count(mask, lane) + 1, 0)
    values = jnp.where(mask > 0, values, 0)
    for b in (1, 2, 4, 8, 16, 32):
        moves = (shift & b) > 0
        values = jnp.where(moves, 0, values) + pltpu.roll(jnp.where(moves, values, 0), 128 - b, 1)
        shift = jnp.where(moves, 0, shift) + pltpu.roll(jnp.where(moves, shift, 0), 128 - b, 1)
    return values


def flip(coordinate, high):
    return 3 - coordinate if high else coordinate ^ 1


def whole_kernel(
    own_ids, tok_in, cot_in, cache_in, wq_in, wk_in, wv_in, ctx_out, grads, *scratch
):
    it = iter(scratch)

    def take(n=None):
        return next(it) if n is None else tuple(next(it) for _ in range(n))

    id_row, ids_shard, id_group, ids_dp, asked_v, slots_v, asked_s, slots_s = take(8)
    cache, tok, cot = take(3)
    weights = take(3)
    wq, wk, wv = weights
    outgoing, replies, chosen = take(3), take(3), take(3)
    lat = take()
    normed, normed_t, q, kb, vb, qg, kg, vg, lat_t, ctx = take(10)
    xs, crecv, acc, snd, rcv = take(5)
    local_sem, id_send, id_recv, gid_send, gid_recv, w_send, w_recv = take(7)
    dp_send, dp_recv, sh_send, sh_recv, send_sem, recv_sem = take(6)

    dp = lax.axis_index("dp")
    shard = lax.axis_index("shard")
    z, x, y, core = dp // 4, dp % 4, shard // 2, shard % 2
    other = (dp, y * 2 + (1 - core))
    pending = []

    def send(src, dst, ss, rs, device):
        copy = pltpu.make_async_remote_copy(
            src_ref=src,
            dst_ref=dst,
            send_sem=ss,
            recv_sem=rs,
            device_id=device,
            device_id_type=MESH,
        )
        copy.start()
        pending.append(copy)
        return copy

    barrier = pltpu.get_barrier_semaphore()
    for r in range(1, 8):
        pl.semaphore_signal(barrier, inc=1, device_id=(dp, shard ^ r), device_id_type=MESH)
    for r in DP_ORDER:
        pl.semaphore_signal(barrier, inc=1, device_id=(dp ^ r, shard), device_id_type=MESH)

    def w_rows(a, row, side, start=0, size=None):
        n = WEIGHT_ROWS[a]
        at = pl.multiple_of((row * 2 + side) * n + start, 16)
        return weights[a].at[pl.ds(at, n if size is None else size)]

    own_weights = []
    for a, src in enumerate((wq_in, wk_in, wv_in)):
        copy = pltpu.make_async_copy(src, w_rows(a, y, core), local_sem.at[a])
        copy.start()
        own_weights.append(copy)
    loads = []
    for n, (src, dst) in enumerate(((cache_in, cache), (tok_in, tok), (cot_in, cot))):
        copy = pltpu.make_async_copy(src, dst, local_sem.at[3 + n])
        copy.start()
        loads.append(copy)

    pl.semaphore_wait(barrier, 22)

    row_lane = lax.broadcasted_iota(jnp.int32, (8, 128), 1)
    own_row = jnp.zeros((8, 128), jnp.int32)
    for k in range(8):
        own_row = jnp.where(row_lane == shard * 8 + k, own_ids[k // 2, k % 2], own_row)
    id_row[...] = own_row
    ids_shard[shard] = own_row
    asks = [
        send(id_row, ids_shard.at[shard], id_send.at[r], id_recv.at[r], (dp, shard ^ r))
        for r in range(1, 8)
    ]
    for copy in asks:
        copy.wait_recv()
    group = ids_shard[0]
    for s in range(1, 8):
        group = group + ids_shard[s]
    id_group[...] = group
    ids_dp[dp] = group
    asks = [
        send(id_group, ids_dp.at[dp], gid_send.at[r], gid_recv.at[r], (dp ^ r, shard))
        for r in DP_ORDER
    ]

    up, down, far = (y + 1) % 4, (y + 3) % 4, (y + 2) % 4
    for copy in own_weights:
        copy.wait()
    kinds = {}

    def send_weights(kind, row, device, part=None):
        copies = []
        for a in range(3):
            n, cut = WEIGHT_ROWS[a], WEIGHT_CUTS[a]
            start, size = ((0, n), (0, cut), (cut, n - cut))[0 if part is None else 1 + part]
            ref = w_rows(a, row, core, start, size)
            copies.append(send(ref, ref, w_send.at[kind, a], w_recv.at[kind, a], device))
        kinds[kind] = copies

    def arrived(kind):
        for copy in kinds[kind]:
            copy.wait_recv()

    send_weights(0, y, (dp, up * 2 + core))
    send_weights(1, y, (dp, down * 2 + core))
    send_weights(2, y, other)

    lane = lax.broadcasted_iota(jnp.int32, (16, 128), 1)
    owners = lax.broadcasted_iota(jnp.int32, (16, 128), 0)
    mine = jnp.where((lane < 64) & ((group[0:1] >> 7) == owners), 1, 0)
    places = jnp.where(mine > 0, owners * 8 + running_count(mine, lane) - 1, 0)
    slots = places[0:1]
    for o in range(1, 16):
        slots = slots + places[o : o + 1]
    slots_v[...] = jnp.broadcast_to(slots, (8, 128))

    for copy in asks:
        copy.wait_recv()
    ids = jnp.concatenate([ids_dp[g][0:1] for g in range(16)], axis=0)
    wanted = jnp.where((lane < 64) & ((ids >> 7) == dp), 1, 0)
    asked_v[...] = packed_left(wanted, ids & 127, lane)
    to_scalar = [
        pltpu.make_async_copy(asked_v, asked_s, local_sem.at[6]),
        pltpu.make_async_copy(slots_v, slots_s, local_sem.at[7]),
    ]
    for copy in to_scalar:
        copy.start()
    loads[0].wait()
    for copy in to_scalar:
        copy.wait()

    @pl.loop(0, 16)
    def _(g):
        for j in range(8):
            row = asked_s[g, j]
            for c, (at, width) in enumerate(CHUNKS):
                outgoing[c][g, j] = cache[row, :, at : at + width]

    fetches = []
    for c in range(3):
        own = pl.ds(pl.multiple_of(dp * 8, 8), 8)
        fetches.append(
            [
                send(
                    outgoing[c].at[dp ^ r],
                    replies[c].at[own],
                    dp_send.at[c, r],
                    dp_recv.at[c, r],
                    (dp ^ r, shard),
                )
                for r in DP_ORDER
            ]
        )
    for c in range(3):
        replies[c][pl.ds(pl.multiple_of(dp * 8, 8), 8)] = outgoing[c][dp]

    loads[1].wait()
    loads[2].wait()

    @pl.loop(0, 8)
    def _(i):
        rows = pl.ds(pl.multiple_of(i * 32, 32), 32)
        t = tok[rows, :].astype(jnp.float32)
        inverse = lax.rsqrt(jnp.mean(t * t, axis=-1, keepdims=True) + 1e-06)
        normed[rows, :] = (t * inverse).astype(jnp.bfloat16)

    eye_wide = one_hot(256, 256, lambda r, c: r == c)

    @pl.loop(0, 8)
    def _(i):
        cols = pl.ds(pl.multiple_of(i * 256, 256), 256)
        normed_t[cols, :] = nt_dot(eye_wide, normed[:, cols]).astype(jnp.bfloat16)

    spread = []

    def hand_on(c):
        at, width = CHUNKS[c]
        for copy in fetches[c]:
            copy.wait_recv()

        @pl.loop(0, 8)
        def _(s):
            for i in range(8):
                chosen[c][s, i] = replies[c][slots_s[0, s * 8 + i]]

        for r in range(1, 8):
            spread.append(
                send(
                    chosen[c].at[shard ^ r],
                    lat.at[:, shard, :, pl.ds(at, width)],
                    sh_send.at[c, r],
                    sh_recv.at[c, r],
                    (dp, shard ^ r),
                )
            )
        lat[:, shard, :, at : at + width] = chosen[c][shard]

    arrived(0)
    send_weights(3, down, (dp, up * 2 + core), 0)
    send_weights(5, down, other)
    arrived(1)
    send_weights(4, up, (dp, down * 2 + core), 1)
    send_weights(6, up, other)
    hand_on(0)
    arrived(3)
    send_weights(7, far, other, 0)
    arrived(4)
    send_weights(8, far, other, 1)
    hand_on(1)
    for kind in (2, 5, 6, 7, 8):
        arrived(kind)

    scale = HEAD_DIM ** (-0.5)

    @pl.loop(0, 4)
    def _(i):
        cols = pl.ds(pl.multiple_of(i * 256, 256), 256)
        q[:, cols] = (nn_dot(normed[...], wq[:, cols]) * scale).astype(jnp.bfloat16)

    def turn_latents(b):
        at, width = ((0, 256), (128, 384), (384, 384), (640, 256))[b]
        pick = one_hot(
            256,
            width,
            lambda r, c: (c + at == 224 * b + 7 * (r >> 3) + (r & 7)) & ((r & 7) < 7),
        )
        for n in range(4):
            block = lat[2 * n : 2 * n + 2, :, :, at : at + width].reshape(256, width)
            lat_t[256 * b : 256 * b + 256, 256 * n : 256 * n + 256] = nt_dot(pick, block).astype(
                jnp.bfloat16
            )

    early = list(spread)
    hand_on(2)
    for copy in early:
        copy.wait_recv()
    for b in range(3):
        turn_latents(b)
    for copy in spread[len(early) :]:
        copy.wait_recv()
    turn_latents(3)

    eye = one_hot(128, 128, lambda r, c: r == c)
    zero = jnp.zeros((SPAN, HEAD_DIM), jnp.bfloat16)

    def diagonal(ref, rows, at):
        a = ref[rows, at : at + HEAD_DIM]
        b = ref[rows, at + HEAD_DIM : at + 2 * HEAD_DIM]
        return jnp.concatenate(
            [jnp.concatenate([a, zero], axis=1), jnp.concatenate([zero, b], axis=1)], axis=0
        )

    @pl.loop(0, CH_DEV)
    def _(c):
        rows = pl.ds(pl.multiple_of(c * 256, 256), 256)
        trows = pl.ds(pl.multiple_of(c * SPAN, SPAN), SPAN)
        block = lat[pl.ds(2 * c, 2)].reshape(256, LAT)
        for at in range(0, INNER, 256):
            kb[:, at : at + 256] = nn_dot(block, wk[:, at : at + 256]).astype(jnp.bfloat16)
            vb[:, at : at + 256] = nn_dot(block, wv[:, at : at + 256]).astype(jnp.bfloat16)
        for at in range(0, INNER, 256):
            mid = at + HEAD_DIM
            end = at + 256
            kp = kb[:, at:end]
            vp = vb[:, at:end]
            q2 = diagonal(q, trows, at)
            g2 = diagonal(cot, trows, at)
            scores = nt_dot(kp, q2)
            e = jnp.exp(scores - jnp.max(scores, axis=0, keepdims=True))
            prob = e * (1.0 / jnp.sum(e, axis=0, keepdims=True))
            prob_t = prob.astype(jnp.bfloat16)
            prob_r = nt_dot(eye, prob_t).astype(jnp.bfloat16)
            c2 = nn_dot(prob_r, vp).astype(jnp.bfloat16)
            ctx[trows, at:mid] = c2[:SPAN, :HEAD_DIM]
            ctx[trows, mid:end] = c2[SPAN:, HEAD_DIM:]
            vg[rows, at:end] = nn_dot(prob_t, g2).astype(jnp.bfloat16)
            pg = nt_dot(vp, g2)
            sg_t = (prob * (pg - jnp.sum(prob * pg, axis=0, keepdims=True))).astype(jnp.bfloat16)
            kg[rows, at:end] = nn_dot(sg_t, q2).astype(jnp.bfloat16)
            sg = nt_dot(eye, sg_t).astype(jnp.bfloat16)
            qg2 = (nn_dot(sg, kp) * scale).astype(jnp.bfloat16)
            qg[trows, at:mid] = qg2[:SPAN, :HEAD_DIM]
            qg[trows, mid:end] = qg2[SPAN:, HEAD_DIM:]

    ctx_copy = pltpu.make_async_copy(ctx, ctx_out, local_sem.at[8])
    ctx_copy.start()

    def across(dims):
        pz, px, py = z, x, y
        for d in dims:
            if d < 2:
                pz = flip(pz, d % 2 == 0)
            elif d < 4:
                px = flip(px, d % 2 == 0)
            else:
                py = flip(py, d % 2 == 0)
        return (pz * 4 + px, py * 2 + core)

    here = place(z * 16 + x * 4 + y, 0)
    coming = [None] * 16
    base = [0] * 16
    root = [0] * 16

    def to_other_core(t):
        coming[t] = send(
            xs.at[t, 1 - core], crecv.at[t], send_sem.at[0, t], recv_sem.at[0, t], other
        )

    def totals(k, t):
        step = min(CHIPS >> (k + 1), 16)

        def summed(at):
            where = pl.ds(at, step)
            if k == 0:
                return xs[t, core, where].astype(jnp.float32) + crecv[t, where].astype(jnp.float32)
            back = pl.ds(OFFSETS[k - 1] + at - base[t], step)
            return acc[t, pl.ds(at - root[t], step)] + rcv[t, back].astype(jnp.float32)

        return summed, step

    def halve(k, t):
        half = CHIPS >> (k + 1)
        d = (TURNS[t] + k) % LEVELS
        bit = (here >> (LEVELS - 1 - d)) & 1
        away = base[t] + (1 - bit) * half
        keep = base[t] + bit * half
        coming[t].wait_recv()
        if k == 0:
            root[t] = keep
        summed, step = totals(k, t)

        @pl.loop(0, half // step)
        def _(i):
            snd[t, pl.ds(OFFSETS[k] + i * step, step)] = summed(away + i * step).astype(
                jnp.bfloat16
            )

        span = pl.ds(OFFSETS[k], half)
        copy = send(
            snd.at[t, span],
            rcv.at[t, span],
            send_sem.at[1 + k, t],
            recv_sem.at[1 + k, t],
            across((d,)),
        )

        @pl.loop(0, half // step)
        def _(i):
            acc[t, pl.ds(keep - root[t] + i * step, step)] = summed(keep + i * step)

        base[t] = keep
        coming[t] = copy

    last = {}

    def exchange_rest(t):
        coming[t].wait_recv()
        whole = acc[t, pl.ds(base[t] - root[t], 8)] + rcv[t, pl.ds(OFFSETS[2], 8)].astype(
            jnp.float32
        )
        acc[t, pl.ds(base[t] - root[t], 8)] = whole
        snd[t, pl.ds(56, 8)] = whole.astype(jnp.bfloat16)
        own = place(z * 16 + x * 4 + y, TURNS[t]) & 7
        last[t] = []
        for m in (4, 2, 1, 6, 5, 3, 7):
            dims = [(TURNS[t] + 3 + e) % LEVELS for e in range(3) if m & (4 >> e)]
            last[t].append(
                send(
                    snd.at[t, 56 + (own ^ m)],
                    rcv.at[t, 56 + m],
                    send_sem.at[4 + m, t],
                    recv_sem.at[4 + m, t],
                    across(dims),
                )
            )

    def finish(t):
        for copy in last[t]:
            copy.wait_recv()
        own = place(z * 16 + x * 4 + y, TURNS[t]) & 7
        total = acc[t, base[t] - root[t] + own]
        for m in range(1, 8):
            total = total + rcv[t, 56 + m].astype(jnp.float32)
        at = 128 * (t % 8)
        grads[16 * (t // 8) : 16 * (t // 8) + 16, at : at + 128] = total

    for n in range(4):

        @pl.loop(0, 4)
        def _(i):
            turned = normed_t[pl.ds(pl.multiple_of(i * 512, 512), 512), :]
            r = nn_dot(turned, qg[:, 256 * n : 256 * n + 256]).astype(jnp.bfloat16)
            for j in range(32):
                for e in range(2):
                    t = 2 * n + e
                    xs[t, j & 1, place(16 * i + (j >> 1), TURNS[t])] = r[
                        16 * j : 16 * j + 16, 128 * e : 128 * e + 128
                    ]

        to_other_core(2 * n)
        to_other_core(2 * n + 1)

    plan = (
        ((0, 0), (0, 1), (0, 2), (0, 3)),
        ((0, 4), (0, 5), (0, 6), (0, 7)),
        ((0, 8), (0, 9), (1, 0), (1, 1), (1, 2), (1, 3)),
        (
            *((0, t) for t in (10, 11)),
            *((1, t) for t in (4, 5, 6, 7)),
            *((0, t) for t in (12, 13)),
            *((2, t) for t in (0, 1, 2, 3)),
            *((0, t) for t in (14, 15)),
            *((1, t) for t in (8, 9, 10, 11)),
            *((2, t) for t in (4, 5, 6, 7)),
            *((3, t) for t in (0, 1, 2, 3)),
            *((1, t) for t in (12, 13, 14, 15)),
            *((2, t) for t in (8, 9, 10, 11)),
            *((3, t) for t in (4, 5, 6, 7)),
            *((2, t) for t in (12, 13, 14, 15)),
            *((3, t) for t in range(8, 16)),
        ),
    )
    for n in range(4):

        @pl.loop(0, 2)
        def _(b):
            turned = lat_t[pl.ds(pl.multiple_of(b * 512, 512), 512), :]
            rk = nn_dot(turned, kg[:, 256 * n : 256 * n + 256])
            rv = nn_dot(turned, vg[:, 256 * n : 256 * n + 256])
            for j in range(64):
                both = jnp.concatenate([rk[8 * j : 8 * j + 8], rv[8 * j : 8 * j + 8]], axis=0)
                both = both.astype(jnp.bfloat16)
                for e in range(2):
                    t = 8 + 2 * n + e
                    xs[t, j & 1, place(32 * b + (j >> 1), TURNS[t])] = both[
                        :, 128 * e : 128 * e + 128
                    ]

        to_other_core(8 + 2 * n)
        to_other_core(9 + 2 * n)
        for k, t in plan[n]:
            if k < 3:
                halve(k, t)
            else:
                exchange_rest(t)
    for t in range(16):
        finish(t)
    ctx_copy.wait()
    for copy in pending:
        copy.wait_send()


def emit_kernel(ctx, grads, ctx_out, gq, gk, gv):
    ctx_out[...] = ctx[...]
    gq[...] = grads[0:16]
    gk[...] = grads[16:23]
    gv[...] = grads[24:31]


def body(tokens, ctx_cotangent, latent_cache, nbr_ids, w_query, w_key, w_value):
    f32, bf, i32 = jnp.float32, jnp.bfloat16, jnp.int32
    vmem = pl.BlockSpec(memory_space=pltpu.VMEM)
    hbm = pl.BlockSpec(memory_space=pl.ANY)
    dma = pltpu.SemaphoreType.DMA
    widths = [w for _, w in CHUNKS]
    context, grads = pl.pallas_call(
        whole_kernel,
        out_shape=(
            jax.ShapeDtypeStruct((256, INNER), bf),
            jax.ShapeDtypeStruct((32, INNER), f32),
        ),
        in_specs=[pl.BlockSpec(memory_space=pltpu.SMEM)] + [hbm] * 6,
        out_specs=(hbm, vmem),
        scratch_shapes=[
            pltpu.VMEM((8, 128), i32),
            pltpu.VMEM((8, 8, 128), i32),
            pltpu.VMEM((8, 128), i32),
            pltpu.VMEM((16, 8, 128), i32),
            pltpu.VMEM((16, 128), i32),
            pltpu.VMEM((8, 128), i32),
            pltpu.SMEM((16, 128), i32),
            pltpu.SMEM((8, 128), i32),
            pltpu.VMEM((128, 16, LAT), bf),
            pltpu.VMEM((256, D), bf),
            pltpu.VMEM((256, INNER), bf),
            pltpu.VMEM((D, INNER), bf),
            pltpu.VMEM((LAT, INNER), bf),
            pltpu.VMEM((LAT, INNER), bf),
            *(pltpu.VMEM((16, 8, 16, w), bf) for w in widths),
            *(pltpu.VMEM((128, 16, w), bf) for w in widths),
            *(pltpu.VMEM((8, 8, 16, w), bf) for w in widths),
            pltpu.VMEM((8, 8, 16, LAT), bf),
            pltpu.VMEM((256, D), bf),
            pltpu.VMEM((D, 256), bf),
            pltpu.VMEM((256, INNER), bf),
            pltpu.VMEM((256, INNER), bf),
            pltpu.VMEM((256, INNER), bf),
            pltpu.VMEM((256, INNER), bf),
            pltpu.VMEM((1024, INNER), bf),
            pltpu.VMEM((1024, INNER), bf),
            pltpu.VMEM((1024, 1024), bf),
            pltpu.VMEM((256, INNER), bf),
            pltpu.VMEM((16, 2, CHIPS, 16, 128), bf),
            pltpu.VMEM((16, CHIPS, 16, 128), bf),
            pltpu.VMEM((16, CHIPS // 2, 16, 128), f32),
            pltpu.VMEM((16, CHIPS, 16, 128), bf),
            pltpu.VMEM((16, CHIPS, 16, 128), bf),
            dma((9,)),
            dma((8,)),
            dma((8,)),
            dma((16,)),
            dma((16,)),
            dma((9, 3)),
            dma((9, 3)),
            dma((3, 16)),
            dma((3, 16)),
            dma((3, 8)),
            dma((3, 8)),
            dma((12, 16)),
            dma((12, 16)),
        ],
        compiler_params=pltpu.CompilerParams(
            collective_id=1, has_side_effects=True, vmem_limit_bytes=67043328
        ),
        name="retro",
    )(
        nbr_ids,
        tokens,
        ctx_cotangent,
        latent_cache,
        w_query,
        w_key,
        w_value,
    )
    return pl.pallas_call(
        emit_kernel,
        out_shape=(
            jax.ShapeDtypeStruct((256, INNER), bf),
            jax.ShapeDtypeStruct((16, INNER), f32),
            jax.ShapeDtypeStruct((7, INNER), f32),
            jax.ShapeDtypeStruct((7, INNER), f32),
        ),
        in_specs=[vmem] * 2,
        out_specs=(vmem,) * 4,
        name="emit",
    )(context, grads)


def solution(mesh):
    return jax.shard_map(
        body,
        mesh=mesh,
        in_specs=(
            P(("dp", "shard"), None),
            P(("dp", "shard"), None),
            P("dp", "shard", None),
            P(("dp", "shard"), None),
            P("shard", None),
            P("shard", None),
            P("shard", None),
        ),
        out_specs=(
            P(("dp", "shard"), None),
            P(("dp", "shard"), None),
            P(("dp", "shard"), None),
            P(("dp", "shard"), None),
        ),
        check_vma=False,
    )
```

```python
import jax
import jax.numpy as jnp
from jax import lax
from jax.experimental import pallas as pl
from jax.experimental.pallas import tpu as pltpu
from jax.sharding import PartitionSpec as P

LAT = 896
HEADS = 8
HEAD_DIM = 128
SPAN = 64
NBR = 2
NT = 128
CH_DEV = 4
INNER = 1024
D = 2048
CHIPS = 64
LEVELS = 6
OFFSETS = (0, 32, 48)
TURNS = (0, 1, 4, 5, 2, 3, 0, 1, 2, 3, 0, 1, 4, 5, 2, 3)
CHUNKS = ((0, 384), (384, 384), (768, 128))
DP_ORDER = (1, 4, 3, 12, 2, 8, 5, 15, 7, 13, 6, 9, 11, 14, 10)
WEIGHT_ROWS = (256, 112, 112)
WEIGHT_CUTS = (128, 64, 48)
NT_DIMS = (((1,), (1,)), ((), ()))
MESH = pl.DeviceIdType.MESH


def nt_dot(a, b):
    return lax.dot_general(a, b, NT_DIMS, preferred_element_type=jnp.float32)


def nn_dot(a, b):
    return jnp.dot(a, b, preferred_element_type=jnp.float32)


def place(chip, part):
    code = chip ^ ((chip >> 1) & 21)
    return ((code << part) | (code >> (LEVELS - part))) & (CHIPS - 1)


def one_hot(rows, columns, wanted):
    r = lax.broadcasted_iota(jnp.int32, (rows, columns), 0)
    c = lax.broadcasted_iota(jnp.int32, (rows, columns), 1)
    return wanted(r, c).astype(jnp.float32).astype(jnp.bfloat16)


def running_count(mask, lane):
    for s in (1, 2, 4, 8, 16, 32):
        mask = mask + jnp.where(lane >= s, pltpu.roll(mask, s, 1), 0)
    return mask


def packed_left(mask, values, lane):
    shift = jnp.where(mask > 0, lane - running_count(mask, lane) + 1, 0)
    values = jnp.where(mask > 0, values, 0)
    for b in (1, 2, 4, 8, 16, 32):
        moves = (shift & b) > 0
        values = jnp.where(moves, 0, values) + pltpu.roll(jnp.where(moves, values, 0), 128 - b, 1)
        shift = jnp.where(moves, 0, shift) + pltpu.roll(jnp.where(moves, shift, 0), 128 - b, 1)
    return values


def flip(coordinate, high):
    return 3 - coordinate if high else coordinate ^ 1


def whole_kernel(
    own_ids, tok_in, cot_in, cache_in, wq_in, wk_in, wv_in, ctx_out, grads, *scratch
):
    it = iter(scratch)

    def take(n=None):
        return next(it) if n is None else tuple(next(it) for _ in range(n))

    id_row, ids_shard, id_group, ids_dp, asked_v, slots_v, asked_s, slots_s = take(8)
    cache, tok, cot = take(3)
    weights = take(3)
    wq, wk, wv = weights
    outgoing, replies, chosen = take(3), take(3), take(3)
    lat = take()
    normed, normed_t, q, qg, kg, vg, lat_t, ctx = take(8)
    xs, crecv, acc, snd, rcv, value_part = take(6)
    local_sem, id_send, id_recv, gid_send, gid_recv, w_send, w_recv = take(7)
    dp_send, dp_recv, sh_send, sh_recv, send_sem, recv_sem = take(6)

    dp = lax.axis_index("dp")
    shard = lax.axis_index("shard")
    z, x, y, core = dp // 4, dp % 4, shard // 2, shard % 2
    other = (dp, y * 2 + (1 - core))
    pending = []

    def send(src, dst, ss, rs, device):
        copy = pltpu.make_async_remote_copy(
            src_ref=src,
            dst_ref=dst,
            send_sem=ss,
            recv_sem=rs,
            device_id=device,
            device_id_type=MESH,
        )
        copy.start()
        pending.append(copy)
        return copy

    barrier = pltpu.get_barrier_semaphore()
    for r in range(1, 8):
        pl.semaphore_signal(barrier, inc=1, device_id=(dp, shard ^ r), device_id_type=MESH)
    for r in DP_ORDER:
        pl.semaphore_signal(barrier, inc=1, device_id=(dp ^ r, shard), device_id_type=MESH)

    def w_rows(a, row, side, start=0, size=None):
        n = WEIGHT_ROWS[a]
        at = pl.multiple_of((row * 2 + side) * n + start, 16)
        return weights[a].at[pl.ds(at, n if size is None else size)]

    own_weights = []
    for a, src in enumerate((wq_in, wk_in, wv_in)):
        copy = pltpu.make_async_copy(src, w_rows(a, y, core), local_sem.at[a])
        copy.start()
        own_weights.append(copy)
    loads = []
    for n, (src, dst) in enumerate(((cache_in, cache), (tok_in, tok), (cot_in, cot))):
        copy = pltpu.make_async_copy(src, dst, local_sem.at[3 + n])
        copy.start()
        loads.append(copy)

    pl.semaphore_wait(barrier, 22)

    row_lane = lax.broadcasted_iota(jnp.int32, (8, 128), 1)
    own_row = jnp.zeros((8, 128), jnp.int32)
    for k in range(8):
        own_row = jnp.where(row_lane == shard * 8 + k, own_ids[k % 2, k // 2], own_row)
    id_row[...] = own_row
    ids_shard[shard] = own_row
    asks = [
        send(id_row, ids_shard.at[shard], id_send.at[r], id_recv.at[r], (dp, shard ^ r))
        for r in range(1, 8)
    ]
    for copy in asks:
        copy.wait_recv()
    group = ids_shard[0]
    for s in range(1, 8):
        group = group + ids_shard[s]
    id_group[...] = group
    ids_dp[dp] = group
    asks = [
        send(id_group, ids_dp.at[dp], gid_send.at[r], gid_recv.at[r], (dp ^ r, shard))
        for r in DP_ORDER
    ]

    up, down, far = (y + 1) % 4, (y + 3) % 4, (y + 2) % 4
    for copy in own_weights:
        copy.wait()
    kinds = {}

    def send_weights(kind, row, device, part=None):
        copies = []
        for a in range(3):
            n, cut = WEIGHT_ROWS[a], WEIGHT_CUTS[a]
            start, size = ((0, n), (0, cut), (cut, n - cut))[0 if part is None else 1 + part]
            ref = w_rows(a, row, core, start, size)
            copies.append(send(ref, ref, w_send.at[kind, a], w_recv.at[kind, a], device))
        kinds[kind] = copies

    def arrived(kind):
        for copy in kinds[kind]:
            copy.wait_recv()

    send_weights(0, y, (dp, up * 2 + core))
    send_weights(1, y, (dp, down * 2 + core))
    send_weights(2, y, other)

    lane = lax.broadcasted_iota(jnp.int32, (16, 128), 1)
    owners = lax.broadcasted_iota(jnp.int32, (16, 128), 0)
    mine = jnp.where((lane < 64) & ((group[0:1] >> 7) == owners), 1, 0)
    places = jnp.where(mine > 0, owners * 8 + running_count(mine, lane) - 1, 0)
    slots = places[0:1]
    for o in range(1, 16):
        slots = slots + places[o : o + 1]
    slots_v[...] = jnp.broadcast_to(slots, (8, 128))

    for copy in asks:
        copy.wait_recv()
    ids = jnp.concatenate([ids_dp[g][0:1] for g in range(16)], axis=0)
    wanted = jnp.where((lane < 64) & ((ids >> 7) == dp), 1, 0)
    asked_v[...] = packed_left(wanted, ids & 127, lane)
    to_scalar = [
        pltpu.make_async_copy(asked_v, asked_s, local_sem.at[6]),
        pltpu.make_async_copy(slots_v, slots_s, local_sem.at[7]),
    ]
    for copy in to_scalar:
        copy.start()
    loads[0].wait()
    for copy in to_scalar:
        copy.wait()

    @pl.loop(0, 16)
    def _(g):
        for j in range(8):
            row = asked_s[g, j]
            for c, (at, width) in enumerate(CHUNKS):
                outgoing[c][g, j] = cache[row, :, at : at + width]

    fetches = []
    for c in range(3):
        own = pl.ds(pl.multiple_of(dp * 8, 8), 8)
        fetches.append(
            [
                send(
                    outgoing[c].at[dp ^ r],
                    replies[c].at[own],
                    dp_send.at[c, r],
                    dp_recv.at[c, r],
                    (dp ^ r, shard),
                )
                for r in DP_ORDER
            ]
        )
    for c in range(3):
        replies[c][pl.ds(pl.multiple_of(dp * 8, 8), 8)] = outgoing[c][dp]

    loads[1].wait()
    loads[2].wait()

    @pl.loop(0, 8)
    def _(i):
        rows = pl.ds(pl.multiple_of(i * 32, 32), 32)
        t = tok[rows, :].astype(jnp.float32)
        inverse = lax.rsqrt(jnp.mean(t * t, axis=-1, keepdims=True) + 1e-06)
        normed[rows, :] = (t * inverse).astype(jnp.bfloat16)

    eye_wide = one_hot(256, 256, lambda r, c: r == c)

    @pl.loop(0, 8)
    def _(i):
        cols = pl.ds(pl.multiple_of(i * 256, 256), 256)
        normed_t[cols, :] = nt_dot(eye_wide, normed[:, cols]).astype(jnp.bfloat16)

    spread = []

    def hand_on(c):
        at, width = CHUNKS[c]
        for copy in fetches[c]:
            copy.wait_recv()

        @pl.loop(0, 8)
        def _(s):
            for i in range(8):
                chosen[c][s, i] = replies[c][slots_s[0, s * 8 + i]]

        for r in range(1, 8):
            spread.append(
                send(
                    chosen[c].at[shard ^ r],
                    lat.at[:, shard, :, pl.ds(at, width)],
                    sh_send.at[c, r],
                    sh_recv.at[c, r],
                    (dp, shard ^ r),
                )
            )
        lat[:, shard, :, at : at + width] = chosen[c][shard]

    def project(c):
        at, width = CHUNKS[c]
        for copy in spread[7 * c : 7 * c + 7]:
            copy.wait_recv()

        @pl.loop(0, CH_DEV)
        def _(n):
            block = lat[pl.ds(2 * n, 2), :, :, at : at + width].reshape(256, width)
            rows = pl.ds(pl.multiple_of((n & 1) * 16, 16), 16)
            for w, total in ((wk, acc), (wv, value_part)):
                for j in range(0, 8, 2):
                    r = nn_dot(block, w[at : at + width, 128 * j : 128 * j + 256])
                    for e in range(2):
                        tile = r[:, 128 * e : 128 * e + 128].reshape(16, 16, 128)
                        index = (n >> 1) * 8 + j + e
                        if c > 0:
                            tile = tile + total[index, rows]
                        total[index, rows] = tile

    arrived(0)
    send_weights(3, down, (dp, up * 2 + core), 0)
    send_weights(5, down, other)
    arrived(1)
    send_weights(4, up, (dp, down * 2 + core), 1)
    send_weights(6, up, other)
    hand_on(0)
    arrived(3)
    send_weights(7, far, other, 0)
    arrived(4)
    send_weights(8, far, other, 1)
    hand_on(1)
    for kind in (2, 5, 6, 7, 8):
        arrived(kind)

    scale = HEAD_DIM ** (-0.5)

    @pl.loop(0, 4)
    def _(i):
        cols = pl.ds(pl.multiple_of(i * 256, 256), 256)
        q[:, cols] = (nn_dot(normed[...], wq[:, cols]) * scale).astype(jnp.bfloat16)

    def turn_latents(b):
        at, width = ((0, 256), (128, 384), (384, 384), (640, 256))[b]
        pick = one_hot(
            256,
            width,
            lambda r, c: (c + at == 224 * b + 7 * (r >> 3) + (r & 7)) & ((r & 7) < 7),
        )
        for n in range(4):
            block = lat[2 * n : 2 * n + 2, :, :, at : at + width].reshape(256, width)
            lat_t[256 * b : 256 * b + 256, 256 * n : 256 * n + 256] = nt_dot(pick, block).astype(
                jnp.bfloat16
            )

    project(0)
    hand_on(2)
    project(1)
    for b in range(3):
        turn_latents(b)
    for copy in spread[14:]:
        copy.wait_recv()
    turn_latents(3)

    eye = one_hot(128, 128, lambda r, c: r == c)
    zero = jnp.zeros((SPAN, HEAD_DIM), jnp.bfloat16)

    def diagonal(ref, rows, at):
        a = ref[rows, at : at + HEAD_DIM]
        b = ref[rows, at + HEAD_DIM : at + 2 * HEAD_DIM]
        return jnp.concatenate(
            [jnp.concatenate([a, zero], axis=1), jnp.concatenate([zero, b], axis=1)], axis=0
        )

    def project_last(w, total, c, at):
        block = lat[2 * c : 2 * c + 2, :, :, 768:LAT].reshape(256, 128)
        r = nn_dot(block, w[768:LAT, at : at + 256])
        tiles = [
            total[(c >> 1) * 8 + at // 128 + e, 16 * (c & 1) : 16 * (c & 1) + 16].reshape(256, 128)
            for e in range(2)
        ]
        return (jnp.concatenate(tiles, axis=1) + r).astype(jnp.bfloat16)

    def attend(at):
        mid = at + HEAD_DIM
        end = at + 256
        for c in range(CH_DEV):
            rows = slice(256 * c, 256 * c + 256)
            trows = slice(SPAN * c, SPAN * c + SPAN)
            kp = project_last(wk, acc, c, at)
            vp = project_last(wv, value_part, c, at)
            q2 = diagonal(q, trows, at)
            g2 = diagonal(cot, trows, at)
            scores = nt_dot(kp, q2)
            e = jnp.exp(scores - jnp.max(scores, axis=0, keepdims=True))
            prob = e * (1.0 / jnp.sum(e, axis=0, keepdims=True))
            prob_t = prob.astype(jnp.bfloat16)
            prob_r = nt_dot(eye, prob_t).astype(jnp.bfloat16)
            c2 = nn_dot(prob_r, vp).astype(jnp.bfloat16)
            ctx[trows, at:mid] = c2[:SPAN, :HEAD_DIM]
            ctx[trows, mid:end] = c2[SPAN:, HEAD_DIM:]
            vg[rows, :] = nn_dot(prob_t, g2).astype(jnp.bfloat16)
            pg = nt_dot(vp, g2)
            sg_t = (prob * (pg - jnp.sum(prob * pg, axis=0, keepdims=True))).astype(jnp.bfloat16)
            kg[rows, :] = nn_dot(sg_t, q2).astype(jnp.bfloat16)
            sg = nt_dot(eye, sg_t).astype(jnp.bfloat16)
            qg2 = (nn_dot(sg, kp) * scale).astype(jnp.bfloat16)
            qg[trows, :HEAD_DIM] = qg2[:SPAN, :HEAD_DIM]
            qg[trows, HEAD_DIM:] = qg2[SPAN:, HEAD_DIM:]

    def across(dims):
        pz, px, py = z, x, y
        for d in dims:
            if d < 2:
                pz = flip(pz, d % 2 == 0)
            elif d < 4:
                px = flip(px, d % 2 == 0)
            else:
                py = flip(py, d % 2 == 0)
        return (pz * 4 + px, py * 2 + core)

    here = place(z * 16 + x * 4 + y, 0)
    coming = [None] * 16
    base = [0] * 16
    root = [0] * 16

    def to_other_core(t):
        coming[t] = send(
            xs.at[t, 1 - core], crecv.at[t], send_sem.at[0, t], recv_sem.at[0, t], other
        )

    def totals(k, t):
        step = min(CHIPS >> (k + 1), 16)

        def summed(at):
            where = pl.ds(at, step)
            if k == 0:
                return xs[t, core, where].astype(jnp.float32) + crecv[t, where].astype(jnp.float32)
            back = pl.ds(OFFSETS[k - 1] + at - base[t], step)
            return acc[t, pl.ds(at - root[t], step)] + rcv[t, back].astype(jnp.float32)

        return summed, step

    def halve(k, t):
        half = CHIPS >> (k + 1)
        d = (TURNS[t] + k) % LEVELS
        bit = (here >> (LEVELS - 1 - d)) & 1
        away = base[t] + (1 - bit) * half
        keep = base[t] + bit * half
        coming[t].wait_recv()
        if k == 0:
            root[t] = keep
        summed, step = totals(k, t)

        @pl.loop(0, half // step)
        def _(i):
            snd[t, pl.ds(OFFSETS[k] + i * step, step)] = summed(away + i * step).astype(
                jnp.bfloat16
            )

        span = pl.ds(OFFSETS[k], half)
        copy = send(
            snd.at[t, span],
            rcv.at[t, span],
            send_sem.at[1 + k, t],
            recv_sem.at[1 + k, t],
            across((d,)),
        )

        @pl.loop(0, half // step)
        def _(i):
            acc[t, pl.ds(keep - root[t] + i * step, step)] = summed(keep + i * step)

        base[t] = keep
        coming[t] = copy

    last = {}

    def exchange_rest(t):
        coming[t].wait_recv()
        whole = acc[t, pl.ds(base[t] - root[t], 8)] + rcv[t, pl.ds(OFFSETS[2], 8)].astype(
            jnp.float32
        )
        acc[t, pl.ds(base[t] - root[t], 8)] = whole
        snd[t, pl.ds(56, 8)] = whole.astype(jnp.bfloat16)
        own = place(z * 16 + x * 4 + y, TURNS[t]) & 7
        last[t] = []
        for m in (4, 2, 1, 6, 5, 3, 7):
            dims = [(TURNS[t] + 3 + e) % LEVELS for e in range(3) if m & (4 >> e)]
            last[t].append(
                send(
                    snd.at[t, 56 + (own ^ m)],
                    rcv.at[t, 56 + m],
                    send_sem.at[4 + m, t],
                    recv_sem.at[4 + m, t],
                    across(dims),
                )
            )

    def finish(t):
        for copy in last[t]:
            copy.wait_recv()
        own = place(z * 16 + x * 4 + y, TURNS[t]) & 7
        total = acc[t, base[t] - root[t] + own]
        for m in range(1, 8):
            total = total + rcv[t, 56 + m].astype(jnp.float32)
        at = 128 * (t % 8)
        grads[16 * (t // 8) : 16 * (t // 8) + 16, at : at + 128] = total

    def query_sums(n):
        @pl.loop(0, 4)
        def _(i):
            turned = normed_t[pl.ds(pl.multiple_of(i * 512, 512), 512), :]
            r = nn_dot(turned, qg[...]).astype(jnp.bfloat16)
            for j in range(32):
                for e in range(2):
                    t = 2 * n + e
                    xs[t, j & 1, place(16 * i + (j >> 1), TURNS[t])] = r[
                        16 * j : 16 * j + 16, 128 * e : 128 * e + 128
                    ]

        to_other_core(2 * n)
        to_other_core(2 * n + 1)

    def latent_sums(n):
        @pl.loop(0, 2)
        def _(b):
            turned = lat_t[pl.ds(pl.multiple_of(b * 512, 512), 512), :]
            rk = nn_dot(turned, kg[...])
            rv = nn_dot(turned, vg[...])
            for j in range(64):
                both = jnp.concatenate([rk[8 * j : 8 * j + 8], rv[8 * j : 8 * j + 8]], axis=0)
                both = both.astype(jnp.bfloat16)
                for e in range(2):
                    t = 8 + 2 * n + e
                    xs[t, j & 1, place(32 * b + (j >> 1), TURNS[t])] = both[
                        :, 128 * e : 128 * e + 128
                    ]

        to_other_core(8 + 2 * n)
        to_other_core(9 + 2 * n)

    def reduce(k, n):
        for t in (2 * n, 2 * n + 1, 8 + 2 * n, 9 + 2 * n):
            if k < 3:
                halve(k, t)
            else:
                exchange_rest(t)

    for n in range(4):
        attend(256 * n)
        if n == 3:
            ctx_copy = pltpu.make_async_copy(ctx, ctx_out, local_sem.at[8])
            ctx_copy.start()
        if n > 0:
            reduce(0, n - 1)
        query_sums(n)
        latent_sums(n)
        for k in range(1, n):
            reduce(k, n - 1 - k)
    for k, n in ((0, 3), (1, 2), (2, 1), (3, 0), (1, 3), (2, 2), (3, 1), (2, 3), (3, 2), (3, 3)):
        reduce(k, n)
    for t in range(16):
        finish(t)
    ctx_copy.wait()
    for copy in pending:
        copy.wait_send()


def emit_kernel(ctx, grads, ctx_out, gq, gk, gv):
    ctx_out[...] = ctx[...]
    gq[...] = grads[0:16]
    gk[...] = grads[16:23]
    gv[...] = grads[24:31]


def body(tokens, ctx_cotangent, latent_cache, nbr_ids, w_query, w_key, w_value):
    f32, bf, i32 = jnp.float32, jnp.bfloat16, jnp.int32
    vmem = pl.BlockSpec(memory_space=pltpu.VMEM)
    hbm = pl.BlockSpec(memory_space=pl.ANY)
    dma = pltpu.SemaphoreType.DMA
    widths = [w for _, w in CHUNKS]
    context, grads = pl.pallas_call(
        whole_kernel,
        out_shape=(
            jax.ShapeDtypeStruct((256, INNER), bf),
            jax.ShapeDtypeStruct((32, INNER), f32),
        ),
        in_specs=[pl.BlockSpec(memory_space=pltpu.SMEM)] + [hbm] * 6,
        out_specs=(hbm, vmem),
        scratch_shapes=[
            pltpu.VMEM((8, 128), i32),
            pltpu.VMEM((8, 8, 128), i32),
            pltpu.VMEM((8, 128), i32),
            pltpu.VMEM((16, 8, 128), i32),
            pltpu.VMEM((16, 128), i32),
            pltpu.VMEM((8, 128), i32),
            pltpu.SMEM((16, 128), i32),
            pltpu.SMEM((8, 128), i32),
            pltpu.VMEM((128, 16, LAT), bf),
            pltpu.VMEM((256, D), bf),
            pltpu.VMEM((256, INNER), bf),
            pltpu.VMEM((D, INNER), bf),
            pltpu.VMEM((LAT, INNER), bf),
            pltpu.VMEM((LAT, INNER), bf),
            *(pltpu.VMEM((16, 8, 16, w), bf) for w in widths),
            *(pltpu.VMEM((128, 16, w), bf) for w in widths),
            *(pltpu.VMEM((8, 8, 16, w), bf) for w in widths),
            pltpu.VMEM((8, 8, 16, LAT), bf),
            pltpu.VMEM((256, D), bf),
            pltpu.VMEM((D, 256), bf),
            pltpu.VMEM((256, INNER), bf),
            pltpu.VMEM((256, 256), bf),
            pltpu.VMEM((1024, 256), bf),
            pltpu.VMEM((1024, 256), bf),
            pltpu.VMEM((1024, 1024), bf),
            pltpu.VMEM((256, INNER), bf),
            pltpu.VMEM((16, 2, CHIPS, 16, 128), bf),
            pltpu.VMEM((16, CHIPS, 16, 128), bf),
            pltpu.VMEM((16, CHIPS // 2, 16, 128), f32),
            pltpu.VMEM((16, CHIPS, 16, 128), bf),
            pltpu.VMEM((16, CHIPS, 16, 128), bf),
            pltpu.VMEM((16, CHIPS // 2, 16, 128), f32),
            dma((9,)),
            dma((8,)),
            dma((8,)),
            dma((16,)),
            dma((16,)),
            dma((9, 3)),
            dma((9, 3)),
            dma((3, 16)),
            dma((3, 16)),
            dma((3, 8)),
            dma((3, 8)),
            dma((12, 16)),
            dma((12, 16)),
        ],
        compiler_params=pltpu.CompilerParams(
            collective_id=1, has_side_effects=True, vmem_limit_bytes=67043328
        ),
        name="retro",
    )(
        nbr_ids.T,
        tokens,
        ctx_cotangent,
        latent_cache,
        w_query,
        w_key,
        w_value,
    )
    return pl.pallas_call(
        emit_kernel,
        out_shape=(
            jax.ShapeDtypeStruct((256, INNER), bf),
            jax.ShapeDtypeStruct((16, INNER), f32),
            jax.ShapeDtypeStruct((7, INNER), f32),
            jax.ShapeDtypeStruct((7, INNER), f32),
        ),
        in_specs=[vmem] * 2,
        out_specs=(vmem,) * 4,
        name="emit",
    )(context, grads)


def solution(mesh):
    return jax.shard_map(
        body,
        mesh=mesh,
        in_specs=(
            P(("dp", "shard"), None),
            P(("dp", "shard"), None),
            P("dp", "shard", None),
            P(("dp", "shard"), None),
            P("shard", None),
            P("shard", None),
            P("shard", None),
        ),
        out_specs=(
            P(("dp", "shard"), None),
            P(("dp", "shard"), None),
            P(("dp", "shard"), None),
            P(("dp", "shard"), None),
        ),
        check_vma=False,
    )
```

```python
import jax
import jax.numpy as jnp
from jax import lax
from jax.experimental import pallas as pl
from jax.experimental.pallas import tpu as pltpu
from jax.sharding import PartitionSpec as P

LAT = 896
HEADS = 8
HEAD_DIM = 128
SPAN = 64
NBR = 2
NT = 128
CH_DEV = 4
INNER = 1024
D = 2048
CHIPS = 64
CHUNKS = ((0, 384), (384, 128), (512, 128), (640, 128), (768, 128))
DP_ORDER = (1, 4, 3, 12, 2, 8, 5, 15, 7, 13, 6, 9, 11, 14, 10)
WEIGHT_ROWS = (256, 112, 112)
WEIGHT_CUTS = (128, 64, 48)
NT_DIMS = (((1,), (1,)), ((), ()))
MESH = pl.DeviceIdType.MESH


def nt_dot(a, b):
    return lax.dot_general(a, b, NT_DIMS, preferred_element_type=jnp.float32)


def nn_dot(a, b):
    return jnp.dot(a, b, preferred_element_type=jnp.float32)


def place(chip, low_first):
    code = chip ^ ((chip >> 1) & 21)
    high = ((code >> 3) & 4) | ((code >> 2) & 2) | ((code >> 1) & 1)
    low = ((code >> 2) & 4) | ((code >> 1) & 2) | (code & 1)
    return (low << 3) | high if low_first else (high << 3) | low


def one_hot(rows, columns, wanted):
    r = lax.broadcasted_iota(jnp.int32, (rows, columns), 0)
    c = lax.broadcasted_iota(jnp.int32, (rows, columns), 1)
    return wanted(r, c).astype(jnp.float32).astype(jnp.bfloat16)


def running_count(mask, lane):
    for s in (1, 2, 4, 8, 16, 32):
        mask = mask + jnp.where(lane >= s, pltpu.roll(mask, s, 1), 0)
    return mask


def packed_left(mask, values, lane):
    shift = jnp.where(mask > 0, lane - running_count(mask, lane) + 1, 0)
    values = jnp.where(mask > 0, values, 0)
    for b in (1, 2, 4, 8, 16, 32):
        moves = (shift & b) > 0
        values = jnp.where(moves, 0, values) + pltpu.roll(jnp.where(moves, values, 0), 128 - b, 1)
        shift = jnp.where(moves, 0, shift) + pltpu.roll(jnp.where(moves, shift, 0), 128 - b, 1)
    return values


def flip(coordinate, high):
    return 3 - coordinate if high else coordinate ^ 1


def whole_kernel(
    own_ids, tok_in, cot_in, cache_in, wq_in, wk_in, wv_in, ctx_out, grads, *scratch
):
    it = iter(scratch)

    def take(n=None):
        return next(it) if n is None else tuple(next(it) for _ in range(n))

    id_row, ids_shard, id_group, ids_dp, asked_v, slots_v, asked_s, slots_s = take(8)
    cache, tok, cot = take(3)
    weights = take(3)
    wq, wk, wv = weights
    outgoing, replies, chosen = take(5), take(5), take(5)
    lat = take()
    normed, normed_t, q, qg, kg, vg, lat_t, ctx = take(8)
    xs, crecv, acc, snd, rcv, value_part = take(6)
    local_sem, id_send, id_recv, gid_send, gid_recv, w_send, w_recv = take(7)
    dp_send, dp_recv, sh_send, sh_recv, send_sem, recv_sem = take(6)

    dp = lax.axis_index("dp")
    shard = lax.axis_index("shard")
    z, x, y, core = dp // 4, dp % 4, shard // 2, shard % 2
    other = (dp, y * 2 + (1 - core))
    pending = []

    def send(src, dst, ss, rs, device):
        copy = pltpu.make_async_remote_copy(
            src_ref=src,
            dst_ref=dst,
            send_sem=ss,
            recv_sem=rs,
            device_id=device,
            device_id_type=MESH,
        )
        copy.start()
        pending.append(copy)
        return copy

    barrier = pltpu.get_barrier_semaphore()
    for r in range(1, 8):
        pl.semaphore_signal(barrier, inc=1, device_id=(dp, shard ^ r), device_id_type=MESH)
    for r in DP_ORDER:
        pl.semaphore_signal(barrier, inc=1, device_id=(dp ^ r, shard), device_id_type=MESH)

    def w_rows(a, row, side, start=0, size=None):
        n = WEIGHT_ROWS[a]
        at = pl.multiple_of((row * 2 + side) * n + start, 16)
        return weights[a].at[pl.ds(at, n if size is None else size)]

    own_weights = []
    for a, src in enumerate((wq_in, wk_in, wv_in)):
        copy = pltpu.make_async_copy(src, w_rows(a, y, core), local_sem.at[a])
        copy.start()
        own_weights.append(copy)
    loads = []
    for n, (src, dst) in enumerate(((cache_in, cache), (tok_in, tok), (cot_in, cot))):
        copy = pltpu.make_async_copy(src, dst, local_sem.at[3 + n])
        copy.start()
        loads.append(copy)

    pl.semaphore_wait(barrier, 22)

    row_lane = lax.broadcasted_iota(jnp.int32, (8, 128), 1)
    own_row = jnp.zeros((8, 128), jnp.int32)
    for k in range(8):
        own_row = jnp.where(row_lane == shard * 8 + k, own_ids[k % 2, k // 2], own_row)
    id_row[...] = own_row
    ids_shard[shard] = own_row
    asks = [
        send(id_row, ids_shard.at[shard], id_send.at[r], id_recv.at[r], (dp, shard ^ r))
        for r in range(1, 8)
    ]
    for copy in asks:
        copy.wait_recv()
    group = ids_shard[0]
    for s in range(1, 8):
        group = group + ids_shard[s]
    id_group[...] = group
    ids_dp[dp] = group
    asks = [
        send(id_group, ids_dp.at[dp], gid_send.at[r], gid_recv.at[r], (dp ^ r, shard))
        for r in DP_ORDER
    ]

    up, down, far = (y + 1) % 4, (y + 3) % 4, (y + 2) % 4
    for copy in own_weights:
        copy.wait()
    kinds = {}

    def send_weights(kind, row, device, part=None):
        copies = []
        for a in range(3):
            n, cut = WEIGHT_ROWS[a], WEIGHT_CUTS[a]
            start, size = ((0, n), (0, cut), (cut, n - cut))[0 if part is None else 1 + part]
            ref = w_rows(a, row, core, start, size)
            copies.append(send(ref, ref, w_send.at[kind, a], w_recv.at[kind, a], device))
        kinds[kind] = copies

    def arrived(kind):
        for copy in kinds[kind]:
            copy.wait_recv()

    send_weights(0, y, (dp, up * 2 + core))
    send_weights(1, y, (dp, down * 2 + core))
    send_weights(2, y, other)

    lane = lax.broadcasted_iota(jnp.int32, (16, 128), 1)
    owners = lax.broadcasted_iota(jnp.int32, (16, 128), 0)
    mine = jnp.where((lane < 64) & ((group[0:1] >> 7) == owners), 1, 0)
    places = jnp.where(mine > 0, owners * 8 + running_count(mine, lane) - 1, 0)
    slots = places[0:1]
    for o in range(1, 16):
        slots = slots + places[o : o + 1]
    slots_v[...] = jnp.broadcast_to(slots, (8, 128))

    for copy in asks:
        copy.wait_recv()
    ids = jnp.concatenate([ids_dp[g][0:1] for g in range(16)], axis=0)
    wanted = jnp.where((lane < 64) & ((ids >> 7) == dp), 1, 0)
    asked_v[...] = packed_left(wanted, ids & 127, lane)
    to_scalar = [
        pltpu.make_async_copy(asked_v, asked_s, local_sem.at[6]),
        pltpu.make_async_copy(slots_v, slots_s, local_sem.at[7]),
    ]
    for copy in to_scalar:
        copy.start()
    loads[0].wait()
    for copy in to_scalar:
        copy.wait()

    @pl.loop(0, 16)
    def _(g):
        for j in range(8):
            row = asked_s[g, j]
            for c, (at, width) in enumerate(CHUNKS):
                outgoing[c][g, j] = cache[row, :, at : at + width]

    fetches = []
    for c in range(len(CHUNKS)):
        own = pl.ds(pl.multiple_of(dp * 8, 8), 8)
        fetches.append(
            [
                send(
                    outgoing[c].at[dp ^ r],
                    replies[c].at[own],
                    dp_send.at[c, r],
                    dp_recv.at[c, r],
                    (dp ^ r, shard),
                )
                for r in DP_ORDER
            ]
        )
    for c in range(len(CHUNKS)):
        replies[c][pl.ds(pl.multiple_of(dp * 8, 8), 8)] = outgoing[c][dp]

    loads[1].wait()
    loads[2].wait()

    @pl.loop(0, 8)
    def _(i):
        rows = pl.ds(pl.multiple_of(i * 32, 32), 32)
        t = tok[rows, :].astype(jnp.float32)
        inverse = lax.rsqrt(jnp.mean(t * t, axis=-1, keepdims=True) + 1e-06)
        normed[rows, :] = (t * inverse).astype(jnp.bfloat16)

    eye_wide = one_hot(256, 256, lambda r, c: r == c)

    @pl.loop(0, 8)
    def _(i):
        cols = pl.ds(pl.multiple_of(i * 256, 256), 256)
        normed_t[cols, :] = nt_dot(eye_wide, normed[:, cols]).astype(jnp.bfloat16)

    spread = []

    def hand_on(c):
        at, width = CHUNKS[c]
        for copy in fetches[c]:
            copy.wait_recv()

        @pl.loop(0, 8)
        def _(s):
            for i in range(8):
                chosen[c][s, i] = replies[c][slots_s[0, s * 8 + i]]

        for r in range(1, 8):
            spread.append(
                send(
                    chosen[c].at[shard ^ r],
                    lat.at[:, shard, :, pl.ds(at, width)],
                    sh_send.at[c, r],
                    sh_recv.at[c, r],
                    (dp, shard ^ r),
                )
            )
        lat[:, shard, :, at : at + width] = chosen[c][shard]

    def project(at, width):
        @pl.loop(0, CH_DEV)
        def _(n):
            block = lat[pl.ds(2 * n, 2), :, :, at : at + width].reshape(256, width)
            rows = pl.ds(pl.multiple_of((n & 1) * 16, 16), 16)
            for w, total in ((wk, acc), (wv, value_part)):
                for j in range(0, 8, 2):
                    r = nn_dot(block, w[at : at + width, 128 * j : 128 * j + 256])
                    for e in range(2):
                        tile = r[:, 128 * e : 128 * e + 128].reshape(16, 16, 128)
                        index = (n >> 1) * 8 + j + e
                        if at > 0:
                            tile = tile + total[index, rows]
                        total[index, rows] = tile

    def landed(c):
        for copy in spread[7 * c : 7 * c + 7]:
            copy.wait_recv()

    arrived(0)
    send_weights(3, down, (dp, up * 2 + core), 0)
    send_weights(5, down, other)
    arrived(1)
    send_weights(4, up, (dp, down * 2 + core), 1)
    send_weights(6, up, other)
    hand_on(0)
    hand_on(1)
    arrived(3)
    send_weights(7, far, other, 0)
    arrived(4)
    send_weights(8, far, other, 1)
    hand_on(2)
    for kind in (2, 5, 6, 7, 8):
        arrived(kind)

    scale = HEAD_DIM ** (-0.5)

    @pl.loop(0, 4)
    def _(i):
        cols = pl.ds(pl.multiple_of(i * 256, 256), 256)
        q[:, cols] = (nn_dot(normed[...], wq[:, cols]) * scale).astype(jnp.bfloat16)

    def turn_latents(b):
        at, width = ((0, 256), (128, 384), (384, 384), (640, 256))[b]
        pick = one_hot(
            256,
            width,
            lambda r, c: (c + at == 224 * b + 7 * (r >> 3) + (r & 7)) & ((r & 7) < 7),
        )
        for n in range(4):
            block = lat[2 * n : 2 * n + 2, :, :, at : at + width].reshape(256, width)
            lat_t[256 * b : 256 * b + 256, 256 * n : 256 * n + 256] = nt_dot(pick, block).astype(
                jnp.bfloat16
            )

    landed(0)
    project(0, 384)
    turn_latents(0)
    hand_on(3)
    landed(1)
    turn_latents(1)
    landed(2)
    project(384, 256)
    hand_on(4)
    landed(3)
    project(640, 128)
    turn_latents(2)
    landed(4)
    turn_latents(3)

    eye = one_hot(128, 128, lambda r, c: r == c)
    zero = jnp.zeros((SPAN, HEAD_DIM), jnp.bfloat16)

    def diagonal(ref, rows, at):
        a = ref[rows, at : at + HEAD_DIM]
        b = ref[rows, at + HEAD_DIM : at + 2 * HEAD_DIM]
        return jnp.concatenate(
            [jnp.concatenate([a, zero], axis=1), jnp.concatenate([zero, b], axis=1)], axis=0
        )

    def project_last(w, total, c, at):
        block = lat[2 * c : 2 * c + 2, :, :, 768:LAT].reshape(256, 128)
        r = nn_dot(block, w[768:LAT, at : at + 256])
        tiles = [
            total[(c >> 1) * 8 + at // 128 + e, 16 * (c & 1) : 16 * (c & 1) + 16].reshape(256, 128)
            for e in range(2)
        ]
        return (jnp.concatenate(tiles, axis=1) + r).astype(jnp.bfloat16)

    def attend(at):
        mid = at + HEAD_DIM
        end = at + 256
        for c in range(CH_DEV):
            rows = slice(256 * c, 256 * c + 256)
            trows = slice(SPAN * c, SPAN * c + SPAN)
            kp = project_last(wk, acc, c, at)
            vp = project_last(wv, value_part, c, at)
            q2 = diagonal(q, trows, at)
            g2 = diagonal(cot, trows, at)
            scores = nt_dot(kp, q2)
            e = jnp.exp(scores - jnp.max(scores, axis=0, keepdims=True))
            prob = e * (1.0 / jnp.sum(e, axis=0, keepdims=True))
            prob_t = prob.astype(jnp.bfloat16)
            prob_r = nt_dot(eye, prob_t).astype(jnp.bfloat16)
            c2 = nn_dot(prob_r, vp).astype(jnp.bfloat16)
            ctx[trows, at:mid] = c2[:SPAN, :HEAD_DIM]
            ctx[trows, mid:end] = c2[SPAN:, HEAD_DIM:]
            vg[rows, :] = nn_dot(prob_t, g2).astype(jnp.bfloat16)
            pg = nt_dot(vp, g2)
            sg_t = (prob * (pg - jnp.sum(prob * pg, axis=0, keepdims=True))).astype(jnp.bfloat16)
            kg[rows, :] = nn_dot(sg_t, q2).astype(jnp.bfloat16)
            sg = nt_dot(eye, sg_t).astype(jnp.bfloat16)
            qg2 = (nn_dot(sg, kp) * scale).astype(jnp.bfloat16)
            qg[trows, :HEAD_DIM] = qg2[:SPAN, :HEAD_DIM]
            qg[trows, HEAD_DIM:] = qg2[SPAN:, HEAD_DIM:]

    def across(dims):
        pz, px, py = z, x, y
        for d in dims:
            if d < 2:
                pz = flip(pz, d % 2 == 0)
            elif d < 4:
                px = flip(px, d % 2 == 0)
            else:
                py = flip(py, d % 2 == 0)
        return (pz * 4 + px, py * 2 + core)

    chip = z * 16 + x * 4 + y
    coming = [None] * 16

    def to_other_core(t):
        coming[t] = [
            send(xs.at[t, 1 - core], crecv.at[t], send_sem.at[0, t], recv_sem.at[0, t], other)
        ]

    def eight(t, second):
        code = place(chip, t & 1)
        high = (t & 1 == 0) != second
        devices = {}
        for m in (7, 6, 5, 3, 4, 2, 1):
            dims = [2 * e + (0 if high else 1) for e in range(3) if m & (4 >> e)]
            devices[m] = across(dims)
        return (code & 7 if second else code >> 3), devices

    def exchange_first(t):
        for copy in coming[t]:
            copy.wait_recv()

        def summed(at, step):
            where = pl.ds(at, step)
            return xs[t, core, where].astype(jnp.float32) + crecv[t, where].astype(jnp.float32)

        @pl.loop(0, 4)
        def _(i):
            snd[t, pl.ds(i * 16, 16)] = summed(i * 16, 16).astype(jnp.bfloat16)

        own, devices = eight(t, False)
        coming[t] = [
            send(
                snd.at[t, pl.ds((own ^ m) * 8, 8)],
                rcv.at[t, pl.ds(8 * m, 8)],
                send_sem.at[m, t],
                recv_sem.at[m, t],
                device,
            )
            for m, device in devices.items()
        ]
        acc[t, pl.ds(0, 8)] = summed(own * 8, 8)

    def exchange_second(t):
        for copy in coming[t]:
            copy.wait_recv()
        whole = acc[t, pl.ds(0, 8)]
        for m in range(1, 8):
            whole = whole + rcv[t, pl.ds(8 * m, 8)].astype(jnp.float32)
        acc[t, pl.ds(0, 8)] = whole
        snd[t, pl.ds(64, 8)] = whole.astype(jnp.bfloat16)
        own, devices = eight(t, True)
        coming[t] = [
            send(
                snd.at[t, 64 + (own ^ m)],
                rcv.at[t, m],
                send_sem.at[7 + m, t],
                recv_sem.at[7 + m, t],
                device,
            )
            for m, device in devices.items()
        ]

    def finish(t):
        for copy in coming[t]:
            copy.wait_recv()
        total = acc[t, place(chip, t & 1) & 7]
        for m in range(1, 8):
            total = total + rcv[t, m].astype(jnp.float32)
        at = 128 * (t % 8)
        grads[16 * (t // 8) : 16 * (t // 8) + 16, at : at + 128] = total

    def query_sums(n):
        @pl.loop(0, 4)
        def _(i):
            turned = normed_t[pl.ds(pl.multiple_of(i * 512, 512), 512), :]
            r = nn_dot(turned, qg[...]).astype(jnp.bfloat16)
            for j in range(32):
                for e in range(2):
                    t = 2 * n + e
                    xs[t, j & 1, place(16 * i + (j >> 1), t & 1)] = r[
                        16 * j : 16 * j + 16, 128 * e : 128 * e + 128
                    ]

        to_other_core(2 * n)
        to_other_core(2 * n + 1)

    def latent_sums(n):
        @pl.loop(0, 2)
        def _(b):
            turned = lat_t[pl.ds(pl.multiple_of(b * 512, 512), 512), :]
            rk = nn_dot(turned, kg[...])
            rv = nn_dot(turned, vg[...])
            for j in range(64):
                both = jnp.concatenate([rk[8 * j : 8 * j + 8], rv[8 * j : 8 * j + 8]], axis=0)
                both = both.astype(jnp.bfloat16)
                for e in range(2):
                    t = 8 + 2 * n + e
                    xs[t, j & 1, place(32 * b + (j >> 1), t & 1)] = both[
                        :, 128 * e : 128 * e + 128
                    ]

        to_other_core(8 + 2 * n)
        to_other_core(9 + 2 * n)

    def parts(n):
        return (2 * n, 2 * n + 1, 8 + 2 * n, 9 + 2 * n)

    for n in range(4):
        attend(256 * n)
        if n == 3:
            ctx_copy = pltpu.make_async_copy(ctx, ctx_out, local_sem.at[8])
            ctx_copy.start()
        if n > 0:
            for t in parts(n - 1):
                exchange_first(t)
        query_sums(n)
        latent_sums(n)
        if n > 1:
            for t in parts(n - 2):
                exchange_second(t)
    for t in parts(3):
        exchange_first(t)
    for n in (2, 3):
        for t in parts(n):
            exchange_second(t)
    for t in range(16):
        finish(t)
    ctx_copy.wait()
    for copy in pending:
        copy.wait_send()


def emit_kernel(ctx, grads, ctx_out, gq, gk, gv):
    ctx_out[...] = ctx[...]
    gq[...] = grads[0:16]
    gk[...] = grads[16:23]
    gv[...] = grads[24:31]


def body(tokens, ctx_cotangent, latent_cache, nbr_ids, w_query, w_key, w_value):
    f32, bf, i32 = jnp.float32, jnp.bfloat16, jnp.int32
    vmem = pl.BlockSpec(memory_space=pltpu.VMEM)
    hbm = pl.BlockSpec(memory_space=pl.ANY)
    dma = pltpu.SemaphoreType.DMA
    widths = [w for _, w in CHUNKS]
    context, grads = pl.pallas_call(
        whole_kernel,
        out_shape=(
            jax.ShapeDtypeStruct((256, INNER), bf),
            jax.ShapeDtypeStruct((32, INNER), f32),
        ),
        in_specs=[pl.BlockSpec(memory_space=pltpu.SMEM)] + [hbm] * 6,
        out_specs=(hbm, vmem),
        scratch_shapes=[
            pltpu.VMEM((8, 128), i32),
            pltpu.VMEM((8, 8, 128), i32),
            pltpu.VMEM((8, 128), i32),
            pltpu.VMEM((16, 8, 128), i32),
            pltpu.VMEM((16, 128), i32),
            pltpu.VMEM((8, 128), i32),
            pltpu.SMEM((16, 128), i32),
            pltpu.SMEM((8, 128), i32),
            pltpu.VMEM((128, 16, LAT), bf),
            pltpu.VMEM((256, D), bf),
            pltpu.VMEM((256, INNER), bf),
            pltpu.VMEM((D, INNER), bf),
            pltpu.VMEM((LAT, INNER), bf),
            pltpu.VMEM((LAT, INNER), bf),
            *(pltpu.VMEM((16, 8, 16, w), bf) for w in widths),
            *(pltpu.VMEM((128, 16, w), bf) for w in widths),
            *(pltpu.VMEM((8, 8, 16, w), bf) for w in widths),
            pltpu.VMEM((8, 8, 16, LAT), bf),
            pltpu.VMEM((256, D), bf),
            pltpu.VMEM((D, 256), bf),
            pltpu.VMEM((256, INNER), bf),
            pltpu.VMEM((256, 256), bf),
            pltpu.VMEM((1024, 256), bf),
            pltpu.VMEM((1024, 256), bf),
            pltpu.VMEM((1024, 1024), bf),
            pltpu.VMEM((256, INNER), bf),
            pltpu.VMEM((16, 2, CHIPS, 16, 128), bf),
            pltpu.VMEM((16, CHIPS, 16, 128), bf),
            pltpu.VMEM((16, CHIPS // 2, 16, 128), f32),
            pltpu.VMEM((16, CHIPS + 8, 16, 128), bf),
            pltpu.VMEM((16, CHIPS, 16, 128), bf),
            pltpu.VMEM((16, CHIPS // 2, 16, 128), f32),
            dma((9,)),
            dma((8,)),
            dma((8,)),
            dma((16,)),
            dma((16,)),
            dma((9, 3)),
            dma((9, 3)),
            dma((5, 16)),
            dma((5, 16)),
            dma((5, 8)),
            dma((5, 8)),
            dma((15, 16)),
            dma((15, 16)),
        ],
        compiler_params=pltpu.CompilerParams(
            collective_id=1, has_side_effects=True, vmem_limit_bytes=67043328
        ),
        name="retro",
    )(
        nbr_ids.T,
        tokens,
        ctx_cotangent,
        latent_cache,
        w_query,
        w_key,
        w_value,
    )
    return pl.pallas_call(
        emit_kernel,
        out_shape=(
            jax.ShapeDtypeStruct((256, INNER), bf),
            jax.ShapeDtypeStruct((16, INNER), f32),
            jax.ShapeDtypeStruct((7, INNER), f32),
            jax.ShapeDtypeStruct((7, INNER), f32),
        ),
        in_specs=[vmem] * 2,
        out_specs=(vmem,) * 4,
        name="emit",
    )(context, grads)


def solution(mesh):
    return jax.shard_map(
        body,
        mesh=mesh,
        in_specs=(
            P(("dp", "shard"), None),
            P(("dp", "shard"), None),
            P("dp", "shard", None),
            P(("dp", "shard"), None),
            P("shard", None),
            P("shard", None),
            P("shard", None),
        ),
        out_specs=(
            P(("dp", "shard"), None),
            P(("dp", "shard"), None),
            P(("dp", "shard"), None),
            P(("dp", "shard"), None),
        ),
        check_vma=False,
    )
```

```python
import jax
import jax.numpy as jnp
from jax import lax
from jax.experimental import pallas as pl
from jax.experimental.pallas import tpu as pltpu
from jax.sharding import PartitionSpec as P

LAT = 896
HEADS = 8
HEAD_DIM = 128
SPAN = 64
NBR = 2
NT = 128
CH_DEV = 4
INNER = 1024
D = 2048
CHIPS = 64
CHUNKS = ((0, 384), (384, 128), (512, 128), (640, 128), (768, 128))
DP_ORDER = (1, 4, 3, 12, 2, 8, 5, 15, 7, 13, 6, 9, 11, 14, 10)
WEIGHT_ROWS = (256, 112, 112)
WEIGHT_CUTS = (128, 64, 48)
NT_DIMS = (((1,), (1,)), ((), ()))
MESH = pl.DeviceIdType.MESH


def nt_dot(a, b):
    return lax.dot_general(a, b, NT_DIMS, preferred_element_type=jnp.float32)


def nn_dot(a, b):
    return jnp.dot(a, b, preferred_element_type=jnp.float32)


def place(chip, low_first):
    code = chip ^ ((chip >> 1) & 21)
    high = ((code >> 3) & 4) | ((code >> 2) & 2) | ((code >> 1) & 1)
    low = ((code >> 2) & 4) | ((code >> 1) & 2) | (code & 1)
    return (low << 3) | high if low_first else (high << 3) | low


def one_hot(rows, columns, wanted):
    r = lax.broadcasted_iota(jnp.int32, (rows, columns), 0)
    c = lax.broadcasted_iota(jnp.int32, (rows, columns), 1)
    return wanted(r, c).astype(jnp.float32).astype(jnp.bfloat16)


def running_count(mask, lane):
    for s in (1, 2, 4, 8, 16, 32):
        mask = mask + jnp.where(lane >= s, pltpu.roll(mask, s, 1), 0)
    return mask


def packed_left(mask, values, lane):
    shift = jnp.where(mask > 0, lane - running_count(mask, lane) + 1, 0)
    values = jnp.where(mask > 0, values, 0)
    for b in (1, 2, 4, 8, 16, 32):
        moves = (shift & b) > 0
        values = jnp.where(moves, 0, values) + pltpu.roll(jnp.where(moves, values, 0), 128 - b, 1)
        shift = jnp.where(moves, 0, shift) + pltpu.roll(jnp.where(moves, shift, 0), 128 - b, 1)
    return values


def flip(coordinate, high):
    return 3 - coordinate if high else coordinate ^ 1


def whole_kernel(
    ids_in, tok_in, cot_in, cache_in, wq_in, wk_in, wv_in, ctx_out, grads, *scratch
):
    it = iter(scratch)

    def take(n=None):
        return next(it) if n is None else tuple(next(it) for _ in range(n))

    own_ids, id_row, ids_shard, id_group, ids_dp, asked_v, slots_v, asked_s, slots_s = take(9)
    cache, tok, cot = take(3)
    weights = take(3)
    wq, wk, wv = weights
    outgoing, replies, chosen = take(5), take(5), take(5)
    lat = take()
    normed, normed_t, q, qg, kg, vg, lat_t, ctx = take(8)
    xs, crecv, acc, snd, rcv, value_part = take(6)
    local_sem, id_sem, w_send, w_recv, dp_send, dp_recv, sh_send, sh_recv = take(8)
    send_sem, core_recv, first_recv, second_recv = take(4)

    dp = lax.axis_index("dp")
    shard = lax.axis_index("shard")
    z, x, y, core = dp // 4, dp % 4, shard // 2, shard % 2
    other = (dp, y * 2 + (1 - core))

    def send(src, dst, ss, rs, device):
        copy = pltpu.make_async_remote_copy(
            src_ref=src,
            dst_ref=dst,
            send_sem=ss,
            recv_sem=rs,
            device_id=device,
            device_id_type=MESH,
        )
        copy.start()

    def all_of(ref, sem, sent=False):
        copy = pltpu.make_async_remote_copy(
            src_ref=ref,
            dst_ref=ref,
            send_sem=sem,
            recv_sem=sem,
            device_id=other,
            device_id_type=MESH,
        )
        if sent:
            copy.wait_send()
        else:
            copy.wait_recv()

    barrier = pltpu.get_barrier_semaphore()
    for r in range(1, 8):
        pl.semaphore_signal(barrier, inc=1, device_id=(dp, shard ^ r), device_id_type=MESH)
    for r in DP_ORDER:
        pl.semaphore_signal(barrier, inc=1, device_id=(dp ^ r, shard), device_id_type=MESH)

    def w_rows(a, row, side, start=0, size=None):
        n = WEIGHT_ROWS[a]
        at = pl.multiple_of((row * 2 + side) * n + start, 16)
        return weights[a].at[pl.ds(at, n if size is None else size)]

    ids_copy = pltpu.make_async_copy(ids_in, own_ids, local_sem.at[9])
    ids_copy.start()
    own_weights = []
    for a, src in enumerate((wq_in, wk_in, wv_in)):
        copy = pltpu.make_async_copy(src, w_rows(a, y, core), local_sem.at[a])
        copy.start()
        own_weights.append(copy)
    loads = []
    for n, (src, dst) in enumerate(((cache_in, cache), (tok_in, tok), (cot_in, cot))):
        copy = pltpu.make_async_copy(src, dst, local_sem.at[3 + n])
        copy.start()
        loads.append(copy)

    ids_copy.wait()
    pl.semaphore_wait(barrier, 22)

    row_lane = lax.broadcasted_iota(jnp.int32, (8, 128), 1)
    own_row = jnp.zeros((8, 128), jnp.int32)
    for k in range(8):
        own_row = jnp.where(row_lane == shard * 8 + k, own_ids[k % 2, k // 2], own_row)
    id_row[...] = own_row
    ids_shard[shard] = own_row
    for r in range(1, 8):
        send(id_row, ids_shard.at[shard], id_sem.at[0], id_sem.at[1], (dp, shard ^ r))
    all_of(ids_shard.at[0:7], id_sem.at[1])
    group = ids_shard[0]
    for s in range(1, 8):
        group = group + ids_shard[s]
    id_group[...] = group
    ids_dp[dp] = group
    for r in DP_ORDER:
        send(id_group, ids_dp.at[dp], id_sem.at[2], id_sem.at[3], (dp ^ r, shard))

    up, down, far = (y + 1) % 4, (y + 3) % 4, (y + 2) % 4
    for copy in own_weights:
        copy.wait()
    ring = {0: 0, 1: 1, 3: 2, 4: 3}

    def send_weights(kind, row, device, part=None):
        for a in range(3):
            n, cut = WEIGHT_ROWS[a], WEIGHT_CUTS[a]
            start, size = ((0, n), (0, cut), (cut, n - cut))[0 if part is None else 1 + part]
            ref = w_rows(a, row, core, start, size)
            send(ref, ref, w_send.at[kind // 4 % 2], w_recv.at[ring.get(kind, 4)], device)

    def arrived(kind):
        all_of(wq.at[0:480] if kind < 2 else wq.at[0:240], w_recv.at[ring[kind]])

    send_weights(0, y, (dp, up * 2 + core))
    send_weights(1, y, (dp, down * 2 + core))
    send_weights(2, y, other)

    lane = lax.broadcasted_iota(jnp.int32, (16, 128), 1)
    owners = lax.broadcasted_iota(jnp.int32, (16, 128), 0)
    mine = jnp.where((lane < 64) & ((group[0:1] >> 7) == owners), 1, 0)
    places = jnp.where(mine > 0, owners * 8 + running_count(mine, lane) - 1, 0)
    slots = places[0:1]
    for o in range(1, 16):
        slots = slots + places[o : o + 1]
    slots_v[...] = jnp.broadcast_to(slots, (8, 128))

    all_of(ids_dp.at[0:15], id_sem.at[3])
    ids = jnp.concatenate([ids_dp[g][0:1] for g in range(16)], axis=0)
    wanted = jnp.where((lane < 64) & ((ids >> 7) == dp), 1, 0)
    asked_v[...] = packed_left(wanted, ids & 127, lane)
    to_scalar = [
        pltpu.make_async_copy(asked_v, asked_s, local_sem.at[6]),
        pltpu.make_async_copy(slots_v, slots_s, local_sem.at[7]),
    ]
    for copy in to_scalar:
        copy.start()
    loads[0].wait()
    for copy in to_scalar:
        copy.wait()

    @pl.loop(0, 16)
    def _(g):
        for j in range(8):
            row = asked_s[g, j]
            for c, (at, width) in enumerate(CHUNKS):
                outgoing[c][g, j] = cache[row, :, at : at + width]

    for c in range(len(CHUNKS)):
        own = pl.ds(pl.multiple_of(dp * 8, 8), 8)
        for r in DP_ORDER:
            send(
                outgoing[c].at[dp ^ r], replies[c].at[own], dp_send, dp_recv.at[c], (dp ^ r, shard)
            )
    for c in range(len(CHUNKS)):
        replies[c][pl.ds(pl.multiple_of(dp * 8, 8), 8)] = outgoing[c][dp]

    loads[1].wait()
    loads[2].wait()

    @pl.loop(0, 8)
    def _(i):
        rows = pl.ds(pl.multiple_of(i * 32, 32), 32)
        t = tok[rows, :].astype(jnp.float32)
        inverse = lax.rsqrt(jnp.mean(t * t, axis=-1, keepdims=True) + 1e-06)
        normed[rows, :] = (t * inverse).astype(jnp.bfloat16)

    eye_wide = one_hot(256, 256, lambda r, c: r == c)

    @pl.loop(0, 8)
    def _(i):
        cols = pl.ds(pl.multiple_of(i * 256, 256), 256)
        normed_t[cols, :] = nt_dot(eye_wide, normed[:, cols]).astype(jnp.bfloat16)

    def hand_on(c):
        at, width = CHUNKS[c]
        all_of(replies[c].at[0:120], dp_recv.at[c])

        @pl.loop(0, 8)
        def _(s):
            for i in range(8):
                chosen[c][s, i] = replies[c][slots_s[0, s * 8 + i]]

        for r in range(1, 8):
            send(
                chosen[c].at[shard ^ r],
                lat.at[:, shard, :, pl.ds(at, width)],
                sh_send,
                sh_recv.at[c],
                (dp, shard ^ r),
            )
        lat[:, shard, :, at : at + width] = chosen[c][shard]

    def project(at, width):
        @pl.loop(0, CH_DEV)
        def _(n):
            block = lat[pl.ds(2 * n, 2), :, :, at : at + width].reshape(256, width)
            rows = pl.ds(pl.multiple_of((n & 1) * 16, 16), 16)
            for w, total in ((wk, acc), (wv, value_part)):
                for j in range(0, 8, 2):
                    r = nn_dot(block, w[at : at + width, 128 * j : 128 * j + 256])
                    for e in range(2):
                        tile = r[:, 128 * e : 128 * e + 128].reshape(16, 16, 128)
                        index = (n >> 1) * 8 + j + e
                        if at > 0:
                            tile = tile + total[index, rows]
                        total[index, rows] = tile

    def landed(c):
        all_of(replies[c].at[0:56], sh_recv.at[c])

    arrived(0)
    send_weights(3, down, (dp, up * 2 + core), 0)
    send_weights(5, down, other)
    arrived(1)
    send_weights(4, up, (dp, down * 2 + core), 1)
    send_weights(6, up, other)
    hand_on(0)
    hand_on(1)
    arrived(3)
    send_weights(7, far, other, 0)
    arrived(4)
    send_weights(8, far, other, 1)
    hand_on(2)
    all_of(wq.at[0:1920], w_recv.at[4])

    scale = HEAD_DIM ** (-0.5)

    @pl.loop(0, 4)
    def _(i):
        cols = pl.ds(pl.multiple_of(i * 256, 256), 256)
        q[:, cols] = (nn_dot(normed[...], wq[:, cols]) * scale).astype(jnp.bfloat16)

    def turn_latents(b):
        at, width = ((0, 256), (128, 384), (384, 384), (640, 256))[b]
        pick = one_hot(
            256,
            width,
            lambda r, c: (c + at == 224 * b + 7 * (r >> 3) + (r & 7)) & ((r & 7) < 7),
        )
        for n in range(4):
            block = lat[2 * n : 2 * n + 2, :, :, at : at + width].reshape(256, width)
            lat_t[256 * b : 256 * b + 256, 256 * n : 256 * n + 256] = nt_dot(pick, block).astype(
                jnp.bfloat16
            )

    landed(0)
    project(0, 384)
    turn_latents(0)
    hand_on(3)
    landed(1)
    turn_latents(1)
    landed(2)
    project(384, 256)
    hand_on(4)
    landed(3)
    project(640, 128)
    turn_latents(2)
    landed(4)
    turn_latents(3)

    eye = one_hot(128, 128, lambda r, c: r == c)
    zero = jnp.zeros((SPAN, HEAD_DIM), jnp.bfloat16)

    def diagonal(ref, rows, at):
        a = ref[rows, at : at + HEAD_DIM]
        b = ref[rows, at + HEAD_DIM : at + 2 * HEAD_DIM]
        return jnp.concatenate(
            [jnp.concatenate([a, zero], axis=1), jnp.concatenate([zero, b], axis=1)], axis=0
        )

    def project_last(w, total, c, at):
        block = lat[2 * c : 2 * c + 2, :, :, 768:LAT].reshape(256, 128)
        r = nn_dot(block, w[768:LAT, at : at + 256])
        tiles = [
            total[(c >> 1) * 8 + at // 128 + e, 16 * (c & 1) : 16 * (c & 1) + 16].reshape(256, 128)
            for e in range(2)
        ]
        return (jnp.concatenate(tiles, axis=1) + r).astype(jnp.bfloat16)

    def attend(at):
        mid = at + HEAD_DIM
        end = at + 256
        for c in range(CH_DEV):
            rows = slice(256 * c, 256 * c + 256)
            trows = slice(SPAN * c, SPAN * c + SPAN)
            kp = project_last(wk, acc, c, at)
            vp = project_last(wv, value_part, c, at)
            q2 = diagonal(q, trows, at)
            g2 = diagonal(cot, trows, at)
            scores = nt_dot(kp, q2)
            e = jnp.exp(scores - jnp.max(scores, axis=0, keepdims=True))
            prob = e * (1.0 / jnp.sum(e, axis=0, keepdims=True))
            prob_t = prob.astype(jnp.bfloat16)
            prob_r = nt_dot(eye, prob_t).astype(jnp.bfloat16)
            c2 = nn_dot(prob_r, vp).astype(jnp.bfloat16)
            ctx[trows, at:mid] = c2[:SPAN, :HEAD_DIM]
            ctx[trows, mid:end] = c2[SPAN:, HEAD_DIM:]
            vg[rows, :] = nn_dot(prob_t, g2).astype(jnp.bfloat16)
            pg = nt_dot(vp, g2)
            sg_t = (prob * (pg - jnp.sum(prob * pg, axis=0, keepdims=True))).astype(jnp.bfloat16)
            kg[rows, :] = nn_dot(sg_t, q2).astype(jnp.bfloat16)
            sg = nt_dot(eye, sg_t).astype(jnp.bfloat16)
            qg2 = (nn_dot(sg, kp) * scale).astype(jnp.bfloat16)
            qg[trows, :HEAD_DIM] = qg2[:SPAN, :HEAD_DIM]
            qg[trows, HEAD_DIM:] = qg2[SPAN:, HEAD_DIM:]

    def across(dims):
        pz, px, py = z, x, y
        for d in dims:
            if d < 2:
                pz = flip(pz, d % 2 == 0)
            elif d < 4:
                px = flip(px, d % 2 == 0)
            else:
                py = flip(py, d % 2 == 0)
        return (pz * 4 + px, py * 2 + core)

    chip = z * 16 + x * 4 + y

    def to_other_core(t):
        send(xs.at[t, 1 - core], crecv.at[t], send_sem.at[0], core_recv.at[t // 2], other)

    def eight(t, second):
        code = place(chip, t & 1)
        high = (t & 1 == 0) != second
        devices = {}
        for m in (7, 6, 5, 3, 4, 2, 1):
            dims = [2 * e + (0 if high else 1) for e in range(3) if m & (4 >> e)]
            devices[m] = across(dims)
        return (code & 7 if second else code >> 3), devices

    def exchange_first(t):
        if t % 2 == 0:
            all_of(crecv.at[0:2], core_recv.at[t // 2])

        def summed(at, step):
            where = pl.ds(at, step)
            return xs[t, core, where].astype(jnp.float32) + crecv[t, where].astype(jnp.float32)

        @pl.loop(0, 4)
        def _(i):
            snd[t, pl.ds(i * 16, 16)] = summed(i * 16, 16).astype(jnp.bfloat16)

        own, devices = eight(t, False)
        for m, device in devices.items():
            send(
                snd.at[t, pl.ds((own ^ m) * 8, 8)],
                rcv.at[t, pl.ds(8 * m, 8)],
                send_sem.at[1],
                first_recv.at[t],
                device,
            )
        acc[t, pl.ds(0, 8)] = summed(own * 8, 8)

    def exchange_second(t):
        all_of(rcv.at[t, 8:64], first_recv.at[t])
        whole = acc[t, pl.ds(0, 8)]
        for m in range(1, 8):
            whole = whole + rcv[t, pl.ds(8 * m, 8)].astype(jnp.float32)
        acc[t, pl.ds(0, 8)] = whole
        snd[t, pl.ds(64, 8)] = whole.astype(jnp.bfloat16)
        own, devices = eight(t, True)
        for m, device in devices.items():
            send(
                snd.at[t, 64 + (own ^ m)],
                rcv.at[t, m],
                send_sem.at[2],
                second_recv.at[t // 2],
                device,
            )

    def finish(t):
        if t % 2 == 0:
            all_of(rcv.at[0:2, 1:8], second_recv.at[t // 2])
        total = acc[t, place(chip, t & 1) & 7]
        for m in range(1, 8):
            total = total + rcv[t, m].astype(jnp.float32)
        at = 128 * (t % 8)
        grads[16 * (t // 8) : 16 * (t // 8) + 16, at : at + 128] = total

    def query_sums(n):
        @pl.loop(0, 4)
        def _(i):
            turned = normed_t[pl.ds(pl.multiple_of(i * 512, 512), 512), :]
            r = nn_dot(turned, qg[...]).astype(jnp.bfloat16)
            for j in range(32):
                for e in range(2):
                    t = 2 * n + e
                    xs[t, j & 1, place(16 * i + (j >> 1), t & 1)] = r[
                        16 * j : 16 * j + 16, 128 * e : 128 * e + 128
                    ]

        to_other_core(2 * n)
        to_other_core(2 * n + 1)

    def latent_sums(n):
        @pl.loop(0, 2)
        def _(b):
            turned = lat_t[pl.ds(pl.multiple_of(b * 512, 512), 512), :]
            rk = nn_dot(turned, kg[...])
            rv = nn_dot(turned, vg[...])
            for j in range(64):
                both = jnp.concatenate([rk[8 * j : 8 * j + 8], rv[8 * j : 8 * j + 8]], axis=0)
                both = both.astype(jnp.bfloat16)
                for e in range(2):
                    t = 8 + 2 * n + e
                    xs[t, j & 1, place(32 * b + (j >> 1), t & 1)] = both[
                        :, 128 * e : 128 * e + 128
                    ]

        to_other_core(8 + 2 * n)
        to_other_core(9 + 2 * n)

    def parts(n):
        return (2 * n, 2 * n + 1, 8 + 2 * n, 9 + 2 * n)

    for n in range(4):
        attend(256 * n)
        if n == 3:
            ctx_copy = pltpu.make_async_copy(ctx, ctx_out, local_sem.at[8])
            ctx_copy.start()
        if n > 0:
            for t in parts(n - 1):
                exchange_first(t)
        query_sums(n)
        latent_sums(n)
        if n > 1:
            for t in parts(n - 2):
                exchange_second(t)
    for t in parts(3):
        exchange_first(t)
    for n in (2, 3):
        for t in parts(n):
            exchange_second(t)
    for t in range(16):
        finish(t)
    ctx_copy.wait()
    for ref, sem in (
        (ids_shard.at[0:7], id_sem.at[0]),
        (ids_dp.at[0:15], id_sem.at[2]),
        (wq.at[0:1920], w_send.at[0]),
        (wq.at[0:1440], w_send.at[1]),
        (cache.at[0:120], dp_send),
        (cache.at[0:56], sh_send),
        (crecv, send_sem.at[0]),
        (snd.at[:, 0:56], send_sem.at[1]),
        (snd.at[:, 0:7], send_sem.at[2]),
    ):
        all_of(ref, sem, sent=True)


def emit_kernel(ctx, grads, ctx_out, gq, gk, gv):
    ctx_out[...] = ctx[...]
    gq[...] = grads[0:16]
    gk[...] = grads[16:23]
    gv[...] = grads[24:31]


def body(tokens, ctx_cotangent, latent_cache, nbr_ids, w_query, w_key, w_value):
    f32, bf, i32 = jnp.float32, jnp.bfloat16, jnp.int32
    vmem = pl.BlockSpec(memory_space=pltpu.VMEM)
    hbm = pl.BlockSpec(memory_space=pl.ANY)
    dma = pltpu.SemaphoreType.DMA
    widths = [w for _, w in CHUNKS]
    context, grads = pl.pallas_call(
        whole_kernel,
        out_shape=(
            jax.ShapeDtypeStruct((256, INNER), bf),
            jax.ShapeDtypeStruct((32, INNER), f32),
        ),
        in_specs=[hbm] * 7,
        out_specs=(hbm, vmem),
        scratch_shapes=[
            pltpu.SMEM((2, 4), i32),
            pltpu.VMEM((8, 128), i32),
            pltpu.VMEM((8, 8, 128), i32),
            pltpu.VMEM((8, 128), i32),
            pltpu.VMEM((16, 8, 128), i32),
            pltpu.VMEM((16, 128), i32),
            pltpu.VMEM((8, 128), i32),
            pltpu.SMEM((16, 128), i32),
            pltpu.SMEM((8, 128), i32),
            pltpu.VMEM((128, 16, LAT), bf),
            pltpu.VMEM((256, D), bf),
            pltpu.VMEM((256, INNER), bf),
            pltpu.VMEM((D, INNER), bf),
            pltpu.VMEM((LAT, INNER), bf),
            pltpu.VMEM((LAT, INNER), bf),
            *(pltpu.VMEM((16, 8, 16, w), bf) for w in widths),
            *(pltpu.VMEM((128, 16, w), bf) for w in widths),
            *(pltpu.VMEM((8, 8, 16, w), bf) for w in widths),
            pltpu.VMEM((8, 8, 16, LAT), bf),
            pltpu.VMEM((256, D), bf),
            pltpu.VMEM((D, 256), bf),
            pltpu.VMEM((256, INNER), bf),
            pltpu.VMEM((256, 256), bf),
            pltpu.VMEM((1024, 256), bf),
            pltpu.VMEM((1024, 256), bf),
            pltpu.VMEM((1024, 1024), bf),
            pltpu.VMEM((256, INNER), bf),
            pltpu.VMEM((16, 2, CHIPS, 16, 128), bf),
            pltpu.VMEM((16, CHIPS, 16, 128), bf),
            pltpu.VMEM((16, CHIPS // 2, 16, 128), f32),
            pltpu.VMEM((16, CHIPS + 8, 16, 128), bf),
            pltpu.VMEM((16, CHIPS, 16, 128), bf),
            pltpu.VMEM((16, CHIPS // 2, 16, 128), f32),
            dma((10,)),
            dma((4,)),
            dma((2,)),
            dma((5,)),
            dma,
            dma((5,)),
            dma,
            dma((5,)),
            dma((3,)),
            dma((8,)),
            dma((16,)),
            dma((8,)),
        ],
        compiler_params=pltpu.CompilerParams(
            collective_id=1, has_side_effects=True, vmem_limit_bytes=67043328
        ),
        name="retro",
    )(
        nbr_ids.T,
        tokens,
        ctx_cotangent,
        latent_cache,
        w_query,
        w_key,
        w_value,
    )
    return pl.pallas_call(
        emit_kernel,
        out_shape=(
            jax.ShapeDtypeStruct((256, INNER), bf),
            jax.ShapeDtypeStruct((16, INNER), f32),
            jax.ShapeDtypeStruct((7, INNER), f32),
            jax.ShapeDtypeStruct((7, INNER), f32),
        ),
        in_specs=[vmem] * 2,
        out_specs=(vmem,) * 4,
        name="emit",
    )(context, grads)


def solution(mesh):
    return jax.shard_map(
        body,
        mesh=mesh,
        in_specs=(
            P(("dp", "shard"), None),
            P(("dp", "shard"), None),
            P("dp", "shard", None),
            P(("dp", "shard"), None),
            P("shard", None),
            P("shard", None),
            P("shard", None),
        ),
        out_specs=(
            P(("dp", "shard"), None),
            P(("dp", "shard"), None),
            P(("dp", "shard"), None),
            P(("dp", "shard"), None),
        ),
        check_vma=False,
    )
```

```python
import jax
import jax.numpy as jnp
from jax import lax
from jax.experimental import pallas as pl
from jax.experimental.pallas import tpu as pltpu
from jax.sharding import PartitionSpec as P

LAT = 896
HEADS = 8
HEAD_DIM = 128
SPAN = 64
NBR = 2
NT = 128
CH_DEV = 4
INNER = 1024
D = 2048
CHIPS = 64
CHUNKS = ((0, 384), (384, 128), (512, 128), (640, 128), (768, 128))
DP_ORDER = (1, 4, 3, 12, 2, 8, 5, 15, 7, 13, 6, 9, 11, 14, 10)
WEIGHT_ROWS = (256, 112, 112)
WEIGHT_CUTS = (128, 64, 48)
NT_DIMS = (((1,), (1,)), ((), ()))
MESH = pl.DeviceIdType.MESH


def nt_dot(a, b):
    return lax.dot_general(a, b, NT_DIMS, preferred_element_type=jnp.float32)


def nn_dot(a, b):
    return jnp.dot(a, b, preferred_element_type=jnp.float32)


def place(chip, low_first):
    code = chip ^ ((chip >> 1) & 21)
    high = ((code >> 3) & 4) | ((code >> 2) & 2) | ((code >> 1) & 1)
    low = ((code >> 2) & 4) | ((code >> 1) & 2) | (code & 1)
    return (low << 3) | high if low_first else (high << 3) | low


def one_hot(rows, columns, wanted):
    r = lax.broadcasted_iota(jnp.int32, (rows, columns), 0)
    c = lax.broadcasted_iota(jnp.int32, (rows, columns), 1)
    return wanted(r, c).astype(jnp.float32).astype(jnp.bfloat16)


def running_count(mask, lane):
    for s in (1, 2, 4, 8, 16, 32):
        mask = mask + jnp.where(lane >= s, pltpu.roll(mask, s, 1), 0)
    return mask


def packed_left(mask, values, lane):
    shift = jnp.where(mask > 0, lane - running_count(mask, lane) + 1, 0)
    values = jnp.where(mask > 0, values, 0)
    for b in (1, 2, 4, 8, 16, 32):
        moves = (shift & b) > 0
        values = jnp.where(moves, 0, values) + pltpu.roll(jnp.where(moves, values, 0), 128 - b, 1)
        shift = jnp.where(moves, 0, shift) + pltpu.roll(jnp.where(moves, shift, 0), 128 - b, 1)
    return values


def flip(coordinate, high):
    return 3 - coordinate if high else coordinate ^ 1


def whole_kernel(
    ids_in, tok_in, cot_in, cache_in, wq_in, wk_in, wv_in, ctx_out, grads, *scratch
):
    it = iter(scratch)

    def take(n=None):
        return next(it) if n is None else tuple(next(it) for _ in range(n))

    own_ids, id_row, ids_shard, id_group, ids_dp, asked_v, slots_v, asked_s, slots_s = take(9)
    cache, tok, cot = take(3)
    weights = take(3)
    wq, wk, wv = weights
    outgoing, replies, chosen = take(5), take(5), take(5)
    lat = take()
    normed, normed_t, q, qg, kg, vg, lat_t, ctx = take(8)
    xs, crecv, acc, snd, rcv, value_part = take(6)
    local_sem, id_sem, w_send, w_recv, dp_send, dp_recv, sh_send, sh_recv = take(8)
    send_sem, core_recv, first_recv, second_recv = take(4)

    dp = lax.axis_index("dp")
    shard = lax.axis_index("shard")
    z, x, y, core = dp // 4, dp % 4, shard // 2, shard % 2
    other = (dp, y * 2 + (1 - core))

    def send(src, dst, ss, rs, device):
        copy = pltpu.make_async_remote_copy(
            src_ref=src,
            dst_ref=dst,
            send_sem=ss,
            recv_sem=rs,
            device_id=device,
            device_id_type=MESH,
        )
        copy.start()

    def all_of(ref, sem, sent=False):
        copy = pltpu.make_async_remote_copy(
            src_ref=ref,
            dst_ref=ref,
            send_sem=sem,
            recv_sem=sem,
            device_id=other,
            device_id_type=MESH,
        )
        if sent:
            copy.wait_send()
        else:
            copy.wait_recv()

    barrier = pltpu.get_barrier_semaphore()
    for r in range(1, 8):
        pl.semaphore_signal(barrier, inc=1, device_id=(dp, shard ^ r), device_id_type=MESH)
    for r in DP_ORDER:
        pl.semaphore_signal(barrier, inc=1, device_id=(dp ^ r, shard), device_id_type=MESH)

    def w_rows(a, row, side, start=0, size=None):
        n = WEIGHT_ROWS[a]
        at = pl.multiple_of((row * 2 + side) * n + start, 16)
        return weights[a].at[pl.ds(at, n if size is None else size)]

    ids_copy = pltpu.make_async_copy(ids_in, own_ids, local_sem.at[9])
    ids_copy.start()
    own_weights = []
    for a, src in enumerate((wq_in, wk_in, wv_in)):
        copy = pltpu.make_async_copy(src, w_rows(a, y, core), local_sem.at[a])
        copy.start()
        own_weights.append(copy)
    loads = []
    for n, (src, dst) in enumerate(((cache_in, cache), (tok_in, tok), (cot_in, cot))):
        copy = pltpu.make_async_copy(src, dst, local_sem.at[3 + n])
        copy.start()
        loads.append(copy)

    ids_copy.wait()
    pl.semaphore_wait(barrier, 22)

    row_lane = lax.broadcasted_iota(jnp.int32, (8, 128), 1)
    own_row = jnp.zeros((8, 128), jnp.int32)
    for k in range(8):
        own_row = jnp.where(row_lane == shard * 8 + k, own_ids[k % 2, k // 2], own_row)
    id_row[...] = own_row
    ids_shard[shard] = own_row
    for r in range(1, 8):
        send(id_row, ids_shard.at[shard], id_sem.at[0], id_sem.at[1], (dp, shard ^ r))
    all_of(ids_shard.at[0:7], id_sem.at[1])
    group = ids_shard[0]
    for s in range(1, 8):
        group = group + ids_shard[s]
    id_group[...] = group
    ids_dp[dp] = group
    for r in DP_ORDER:
        send(id_group, ids_dp.at[dp], id_sem.at[2], id_sem.at[3], (dp ^ r, shard))

    up, down, far = (y + 1) % 4, (y + 3) % 4, (y + 2) % 4
    for copy in own_weights:
        copy.wait()
    ring = {0: 0, 1: 1, 3: 2, 4: 3}

    def send_weights(kind, row, device, part=None):
        for a in range(3):
            n, cut = WEIGHT_ROWS[a], WEIGHT_CUTS[a]
            start, size = ((0, n), (0, cut), (cut, n - cut))[0 if part is None else 1 + part]
            ref = w_rows(a, row, core, start, size)
            send(ref, ref, w_send.at[kind // 4 % 2], w_recv.at[ring.get(kind, 4)], device)

    def arrived(kind):
        all_of(wq.at[0:480] if kind < 2 else wq.at[0:240], w_recv.at[ring[kind]])

    send_weights(0, y, (dp, up * 2 + core))
    send_weights(1, y, (dp, down * 2 + core))
    send_weights(2, y, other)

    lane = lax.broadcasted_iota(jnp.int32, (16, 128), 1)
    owners = lax.broadcasted_iota(jnp.int32, (16, 128), 0)
    mine = jnp.where((lane < 64) & ((group[0:1] >> 7) == owners), 1, 0)
    places = jnp.where(mine > 0, owners * 8 + running_count(mine, lane) - 1, 0)
    slots = places[0:1]
    for o in range(1, 16):
        slots = slots + places[o : o + 1]
    slots_v[...] = jnp.broadcast_to(slots, (8, 128))

    all_of(ids_dp.at[0:15], id_sem.at[3])
    ids = jnp.concatenate([ids_dp[g][0:1] for g in range(16)], axis=0)
    wanted = jnp.where((lane < 64) & ((ids >> 7) == dp), 1, 0)
    asked_v[...] = packed_left(wanted, ids & 127, lane)
    to_scalar = [
        pltpu.make_async_copy(asked_v, asked_s, local_sem.at[6]),
        pltpu.make_async_copy(slots_v, slots_s, local_sem.at[7]),
    ]
    for copy in to_scalar:
        copy.start()
    loads[0].wait()
    for copy in to_scalar:
        copy.wait()

    @pl.loop(0, 16)
    def _(g):
        for j in range(8):
            row = asked_s[g, j]
            for c, (at, width) in enumerate(CHUNKS):
                outgoing[c][g, j] = cache[row, :, at : at + width]

    for c in range(len(CHUNKS)):
        own = pl.ds(pl.multiple_of(dp * 8, 8), 8)
        for r in DP_ORDER:
            send(
                outgoing[c].at[dp ^ r], replies[c].at[own], dp_send, dp_recv.at[c], (dp ^ r, shard)
            )
    for c in range(len(CHUNKS)):
        replies[c][pl.ds(pl.multiple_of(dp * 8, 8), 8)] = outgoing[c][dp]

    loads[1].wait()
    loads[2].wait()

    @pl.loop(0, 8)
    def _(i):
        rows = pl.ds(pl.multiple_of(i * 32, 32), 32)
        t = tok[rows, :].astype(jnp.float32)
        inverse = lax.rsqrt(jnp.mean(t * t, axis=-1, keepdims=True) + 1e-06)
        normed[rows, :] = (t * inverse).astype(jnp.bfloat16)

    eye_wide = one_hot(256, 256, lambda r, c: r == c)

    @pl.loop(0, 8)
    def _(i):
        cols = pl.ds(pl.multiple_of(i * 256, 256), 256)
        normed_t[cols, :] = nt_dot(eye_wide, normed[:, cols]).astype(jnp.bfloat16)

    def hand_on(c):
        at, width = CHUNKS[c]
        all_of(replies[c].at[0:120], dp_recv.at[c])

        @pl.loop(0, 8)
        def _(s):
            for i in range(8):
                chosen[c][s, i] = replies[c][slots_s[0, s * 8 + i]]

        for r in range(1, 8):
            send(
                chosen[c].at[shard ^ r],
                lat.at[:, shard, :, pl.ds(at, width)],
                sh_send,
                sh_recv.at[c],
                (dp, shard ^ r),
            )
        lat[:, shard, :, at : at + width] = chosen[c][shard]

    def project(at, width):
        @pl.loop(0, CH_DEV)
        def _(n):
            block = lat[pl.ds(2 * n, 2), :, :, at : at + width].reshape(256, width)
            rows = pl.ds(pl.multiple_of((n & 1) * 16, 16), 16)
            for w, total in ((wk, acc), (wv, value_part)):
                for j in range(0, 8, 2):
                    r = nn_dot(block, w[at : at + width, 128 * j : 128 * j + 256])
                    for e in range(2):
                        tile = r[:, 128 * e : 128 * e + 128].reshape(16, 16, 128)
                        index = (n >> 1) * 8 + j + e
                        if at > 0:
                            tile = tile + total[index, rows]
                        total[index, rows] = tile

    def landed(c):
        all_of(replies[c].at[0:56], sh_recv.at[c])

    arrived(0)
    send_weights(3, down, (dp, up * 2 + core), 0)
    send_weights(5, down, other)
    arrived(1)
    send_weights(4, up, (dp, down * 2 + core), 1)
    send_weights(6, up, other)
    hand_on(0)
    hand_on(1)
    arrived(3)
    send_weights(7, far, other, 0)
    arrived(4)
    send_weights(8, far, other, 1)
    hand_on(2)
    all_of(wq.at[0:1920], w_recv.at[4])

    scale = HEAD_DIM ** (-0.5)

    @pl.loop(0, 4)
    def _(i):
        cols = pl.ds(pl.multiple_of(i * 256, 256), 256)
        q[:, cols] = (nn_dot(normed[...], wq[:, cols]) * scale).astype(jnp.bfloat16)

    def turn_latents(b):
        at, width = ((0, 256), (128, 384), (384, 384), (640, 256))[b]
        pick = one_hot(
            256,
            width,
            lambda r, c: (c + at == 224 * b + 7 * (r >> 3) + (r & 7)) & ((r & 7) < 7),
        )
        for n in range(4):
            block = lat[2 * n : 2 * n + 2, :, :, at : at + width].reshape(256, width)
            lat_t[256 * b : 256 * b + 256, 256 * n : 256 * n + 256] = nt_dot(pick, block).astype(
                jnp.bfloat16
            )

    landed(0)
    project(0, 384)
    turn_latents(0)
    hand_on(3)
    landed(1)
    turn_latents(1)
    hand_on(4)
    landed(2)
    project(384, 256)
    landed(3)
    project(640, 128)
    turn_latents(2)
    landed(4)
    turn_latents(3)

    eye = one_hot(128, 128, lambda r, c: r == c)
    zero = jnp.zeros((SPAN, HEAD_DIM), jnp.bfloat16)

    def diagonal(ref, rows, at):
        a = ref[rows, at : at + HEAD_DIM]
        b = ref[rows, at + HEAD_DIM : at + 2 * HEAD_DIM]
        return jnp.concatenate(
            [jnp.concatenate([a, zero], axis=1), jnp.concatenate([zero, b], axis=1)], axis=0
        )

    def project_last(w, total, c, at):
        block = lat[2 * c : 2 * c + 2, :, :, 768:LAT].reshape(256, 128)
        r = nn_dot(block, w[768:LAT, at : at + 256])
        tiles = [
            total[(c >> 1) * 8 + at // 128 + e, 16 * (c & 1) : 16 * (c & 1) + 16].reshape(256, 128)
            for e in range(2)
        ]
        return (jnp.concatenate(tiles, axis=1) + r).astype(jnp.bfloat16)

    def attend(at):
        mid = at + HEAD_DIM
        end = at + 256
        for c in range(CH_DEV):
            rows = slice(256 * c, 256 * c + 256)
            trows = slice(SPAN * c, SPAN * c + SPAN)
            kp = project_last(wk, acc, c, at)
            vp = project_last(wv, value_part, c, at)
            q2 = diagonal(q, trows, at)
            g2 = diagonal(cot, trows, at)
            scores = nt_dot(kp, q2)
            e = jnp.exp(scores - jnp.max(scores, axis=0, keepdims=True))
            prob = e * (1.0 / jnp.sum(e, axis=0, keepdims=True))
            prob_t = prob.astype(jnp.bfloat16)
            prob_r = nt_dot(eye, prob_t).astype(jnp.bfloat16)
            c2 = nn_dot(prob_r, vp).astype(jnp.bfloat16)
            ctx[trows, at:mid] = c2[:SPAN, :HEAD_DIM]
            ctx[trows, mid:end] = c2[SPAN:, HEAD_DIM:]
            vg[rows, :] = nn_dot(prob_t, g2).astype(jnp.bfloat16)
            pg = nt_dot(vp, g2)
            sg_t = (prob * (pg - jnp.sum(prob * pg, axis=0, keepdims=True))).astype(jnp.bfloat16)
            kg[rows, :] = nn_dot(sg_t, q2).astype(jnp.bfloat16)
            sg = nt_dot(eye, sg_t).astype(jnp.bfloat16)
            qg2 = (nn_dot(sg, kp) * scale).astype(jnp.bfloat16)
            qg[trows, :HEAD_DIM] = qg2[:SPAN, :HEAD_DIM]
            qg[trows, HEAD_DIM:] = qg2[SPAN:, HEAD_DIM:]

    def across(dims):
        pz, px, py = z, x, y
        for d in dims:
            if d < 2:
                pz = flip(pz, d % 2 == 0)
            elif d < 4:
                px = flip(px, d % 2 == 0)
            else:
                py = flip(py, d % 2 == 0)
        return (pz * 4 + px, py * 2 + core)

    chip = z * 16 + x * 4 + y

    def to_other_core(t):
        send(xs.at[t, 1 - core], crecv.at[t], send_sem.at[0], core_recv.at[t // 2], other)

    def eight(t, second):
        code = place(chip, t & 1)
        high = (t & 1 == 0) != second
        devices = {}
        for m in (7, 6, 5, 3, 4, 2, 1):
            dims = [2 * e + (0 if high else 1) for e in range(3) if m & (4 >> e)]
            devices[m] = across(dims)
        return (code & 7 if second else code >> 3), devices

    def exchange_first(t):
        if t % 2 == 0:
            all_of(crecv.at[0:2], core_recv.at[t // 2])

        def summed(at, step):
            where = pl.ds(at, step)
            return xs[t, core, where].astype(jnp.float32) + crecv[t, where].astype(jnp.float32)

        @pl.loop(0, 4)
        def _(i):
            snd[t, pl.ds(i * 16, 16)] = summed(i * 16, 16).astype(jnp.bfloat16)

        own, devices = eight(t, False)
        for m, device in devices.items():
            send(
                snd.at[t, pl.ds((own ^ m) * 8, 8)],
                rcv.at[t, pl.ds(8 * m, 8)],
                send_sem.at[1],
                first_recv.at[t],
                device,
            )
        acc[t, pl.ds(0, 8)] = summed(own * 8, 8)

    def exchange_second(t):
        all_of(rcv.at[t, 8:64], first_recv.at[t])
        whole = acc[t, pl.ds(0, 8)]
        for m in range(1, 8):
            whole = whole + rcv[t, pl.ds(8 * m, 8)].astype(jnp.float32)
        acc[t, pl.ds(0, 8)] = whole
        snd[t, pl.ds(64, 8)] = whole.astype(jnp.bfloat16)
        own, devices = eight(t, True)
        for m, device in devices.items():
            send(
                snd.at[t, 64 + (own ^ m)],
                rcv.at[t, m],
                send_sem.at[2],
                second_recv.at[t // 2],
                device,
            )

    def finish(t):
        if t % 2 == 0:
            all_of(rcv.at[0:2, 1:8], second_recv.at[t // 2])
        total = acc[t, place(chip, t & 1) & 7]
        for m in range(1, 8):
            total = total + rcv[t, m].astype(jnp.float32)
        at = 128 * (t % 8)
        grads[16 * (t // 8) : 16 * (t // 8) + 16, at : at + 128] = total

    def query_sums(n):
        @pl.loop(0, 4)
        def _(i):
            turned = normed_t[pl.ds(pl.multiple_of(i * 512, 512), 512), :]
            r = nn_dot(turned, qg[...]).astype(jnp.bfloat16)
            start = [place(16 * i, e) for e in range(2)]
            for j in range(32):
                for e in range(2):
                    t = 2 * n + e
                    xs[t, j & 1, start[e] ^ place(j >> 1, e)] = r[
                        16 * j : 16 * j + 16, 128 * e : 128 * e + 128
                    ]

        to_other_core(2 * n)
        to_other_core(2 * n + 1)

    def latent_sums(n):
        @pl.loop(0, 2)
        def _(b):
            turned = lat_t[pl.ds(pl.multiple_of(b * 512, 512), 512), :]
            rk = nn_dot(turned, kg[...])
            rv = nn_dot(turned, vg[...])
            start = [place(32 * b, e) for e in range(2)]
            for j in range(64):
                both = jnp.concatenate([rk[8 * j : 8 * j + 8], rv[8 * j : 8 * j + 8]], axis=0)
                both = both.astype(jnp.bfloat16)
                for e in range(2):
                    t = 8 + 2 * n + e
                    xs[t, j & 1, start[e] ^ place(j >> 1, e)] = both[
                        :, 128 * e : 128 * e + 128
                    ]

        to_other_core(8 + 2 * n)
        to_other_core(9 + 2 * n)

    def parts(n):
        return (2 * n, 2 * n + 1, 8 + 2 * n, 9 + 2 * n)

    for n in range(4):
        attend(256 * n)
        if n == 3:
            ctx_copy = pltpu.make_async_copy(ctx, ctx_out, local_sem.at[8])
            ctx_copy.start()
        if n > 0:
            for t in parts(n - 1):
                exchange_first(t)
        query_sums(n)
        latent_sums(n)
        if n == 2:
            for t in parts(0):
                exchange_second(t)
    for t in parts(3):
        exchange_first(t)
    for n in (1, 2, 3):
        for t in parts(n):
            exchange_second(t)
    for t in range(16):
        finish(t)
    ctx_copy.wait()
    for ref, sem in (
        (ids_shard.at[0:7], id_sem.at[0]),
        (ids_dp.at[0:15], id_sem.at[2]),
        (wq.at[0:1920], w_send.at[0]),
        (wq.at[0:1440], w_send.at[1]),
        (cache.at[0:120], dp_send),
        (cache.at[0:56], sh_send),
        (crecv, send_sem.at[0]),
        (snd.at[:, 0:56], send_sem.at[1]),
        (snd.at[:, 0:7], send_sem.at[2]),
    ):
        all_of(ref, sem, sent=True)


def emit_kernel(ctx, grads, ctx_out, gq, gk, gv):
    ctx_out[...] = ctx[...]
    gq[...] = grads[0:16]
    gk[...] = grads[16:23]
    gv[...] = grads[24:31]


def body(tokens, ctx_cotangent, latent_cache, nbr_ids, w_query, w_key, w_value):
    f32, bf, i32 = jnp.float32, jnp.bfloat16, jnp.int32
    vmem = pl.BlockSpec(memory_space=pltpu.VMEM)
    hbm = pl.BlockSpec(memory_space=pl.ANY)
    dma = pltpu.SemaphoreType.DMA
    widths = [w for _, w in CHUNKS]
    context, grads = pl.pallas_call(
        whole_kernel,
        out_shape=(
            jax.ShapeDtypeStruct((256, INNER), bf),
            jax.ShapeDtypeStruct((32, INNER), f32),
        ),
        in_specs=[hbm] * 7,
        out_specs=(hbm, vmem),
        scratch_shapes=[
            pltpu.SMEM((2, 4), i32),
            pltpu.VMEM((8, 128), i32),
            pltpu.VMEM((8, 8, 128), i32),
            pltpu.VMEM((8, 128), i32),
            pltpu.VMEM((16, 8, 128), i32),
            pltpu.VMEM((16, 128), i32),
            pltpu.VMEM((8, 128), i32),
            pltpu.SMEM((16, 128), i32),
            pltpu.SMEM((8, 128), i32),
            pltpu.VMEM((128, 16, LAT), bf),
            pltpu.VMEM((256, D), bf),
            pltpu.VMEM((256, INNER), bf),
            pltpu.VMEM((D, INNER), bf),
            pltpu.VMEM((LAT, INNER), bf),
            pltpu.VMEM((LAT, INNER), bf),
            *(pltpu.VMEM((16, 8, 16, w), bf) for w in widths),
            *(pltpu.VMEM((128, 16, w), bf) for w in widths),
            *(pltpu.VMEM((8, 8, 16, w), bf) for w in widths),
            pltpu.VMEM((8, 8, 16, LAT), bf),
            pltpu.VMEM((256, D), bf),
            pltpu.VMEM((D, 256), bf),
            pltpu.VMEM((256, INNER), bf),
            pltpu.VMEM((256, 256), bf),
            pltpu.VMEM((1024, 256), bf),
            pltpu.VMEM((1024, 256), bf),
            pltpu.VMEM((1024, 1024), bf),
            pltpu.VMEM((256, INNER), bf),
            pltpu.VMEM((16, 2, CHIPS, 16, 128), bf),
            pltpu.VMEM((16, CHIPS, 16, 128), bf),
            pltpu.VMEM((16, CHIPS // 2, 16, 128), f32),
            pltpu.VMEM((16, CHIPS + 8, 16, 128), bf),
            pltpu.VMEM((16, CHIPS, 16, 128), bf),
            pltpu.VMEM((16, CHIPS // 2, 16, 128), f32),
            dma((10,)),
            dma((4,)),
            dma((2,)),
            dma((5,)),
            dma,
            dma((5,)),
            dma,
            dma((5,)),
            dma((3,)),
            dma((8,)),
            dma((16,)),
            dma((8,)),
        ],
        compiler_params=pltpu.CompilerParams(
            collective_id=1, has_side_effects=True, vmem_limit_bytes=67043328
        ),
        name="retro",
    )(
        nbr_ids.T,
        tokens,
        ctx_cotangent,
        latent_cache,
        w_query,
        w_key,
        w_value,
    )
    return pl.pallas_call(
        emit_kernel,
        out_shape=(
            jax.ShapeDtypeStruct((256, INNER), bf),
            jax.ShapeDtypeStruct((16, INNER), f32),
            jax.ShapeDtypeStruct((7, INNER), f32),
            jax.ShapeDtypeStruct((7, INNER), f32),
        ),
        in_specs=[vmem] * 2,
        out_specs=(vmem,) * 4,
        name="emit",
    )(context, grads)


def solution(mesh):
    return jax.shard_map(
        body,
        mesh=mesh,
        in_specs=(
            P(("dp", "shard"), None),
            P(("dp", "shard"), None),
            P("dp", "shard", None),
            P(("dp", "shard"), None),
            P("shard", None),
            P("shard", None),
            P("shard", None),
        ),
        out_specs=(
            P(("dp", "shard"), None),
            P(("dp", "shard"), None),
            P(("dp", "shard"), None),
            P(("dp", "shard"), None),
        ),
        check_vma=False,
    )
```

```python
import jax
import jax.numpy as jnp
from jax import lax
from jax.experimental import pallas as pl
from jax.experimental.pallas import tpu as pltpu
from jax.sharding import PartitionSpec as P

LAT = 896
HEADS = 8
HEAD_DIM = 128
SPAN = 64
NBR = 2
NT = 128
CH_DEV = 4
INNER = 1024
D = 2048
CHIPS = 64
CHUNKS = ((0, 384), (384, 128), (512, 128), (640, 128), (768, 128))
DP_ORDER = (1, 4, 3, 12, 2, 8, 5, 15, 7, 13, 6, 9, 11, 14, 10)
WEIGHT_ROWS = (256, 112, 112)
WEIGHT_CUTS = (128, 64, 48)
NT_DIMS = (((1,), (1,)), ((), ()))
MESH = pl.DeviceIdType.MESH


def nt_dot(a, b):
    return lax.dot_general(a, b, NT_DIMS, preferred_element_type=jnp.float32)


def nn_dot(a, b):
    return jnp.dot(a, b, preferred_element_type=jnp.float32)


def place(chip, low_first):
    code = chip ^ ((chip >> 1) & 21)
    high = ((code >> 3) & 4) | ((code >> 2) & 2) | ((code >> 1) & 1)
    low = ((code >> 2) & 4) | ((code >> 1) & 2) | (code & 1)
    return (low << 3) | high if low_first else (high << 3) | low


def one_hot(rows, columns, wanted):
    r = lax.broadcasted_iota(jnp.int32, (rows, columns), 0)
    c = lax.broadcasted_iota(jnp.int32, (rows, columns), 1)
    return wanted(r, c).astype(jnp.float32).astype(jnp.bfloat16)


def running_count(mask, lane):
    for s in (1, 2, 4, 8, 16, 32):
        mask = mask + jnp.where(lane >= s, pltpu.roll(mask, s, 1), 0)
    return mask


def packed_left(mask, values, lane):
    shift = jnp.where(mask > 0, lane - running_count(mask, lane) + 1, 0)
    values = jnp.where(mask > 0, values, 0)
    for b in (1, 2, 4, 8, 16, 32):
        moves = (shift & b) > 0
        values = jnp.where(moves, 0, values) + pltpu.roll(jnp.where(moves, values, 0), 128 - b, 1)
        shift = jnp.where(moves, 0, shift) + pltpu.roll(jnp.where(moves, shift, 0), 128 - b, 1)
    return values


def flip(coordinate, high):
    return 3 - coordinate if high else coordinate ^ 1


def whole_kernel(
    ids_in, tok_in, cot_in, cache_in, wq_in, wk_in, wv_in, ctx_out, grads, *scratch
):
    it = iter(scratch)

    def take(n=None):
        return next(it) if n is None else tuple(next(it) for _ in range(n))

    own_ids, id_row, ids_shard, id_group, ids_dp, asked_v, slots_v, asked_s, slots_s = take(9)
    cache, tok, cot = take(3)
    weights = take(3)
    wq, wk, wv = weights
    outgoing, replies, chosen = take(5), take(5), take(5)
    lat = take()
    normed, normed_t, q, qg, kg, vg, lat_t, ctx = take(8)
    xs, crecv, acc, snd, rcv, value_part = take(6)
    local_sem, id_sem, w_send, w_recv, dp_send, dp_recv, sh_send, sh_recv = take(8)
    send_sem, core_recv, first_recv, second_recv = take(4)

    dp = lax.axis_index("dp")
    shard = lax.axis_index("shard")
    z, x, y, core = dp // 4, dp % 4, shard // 2, shard % 2
    other = (dp, y * 2 + (1 - core))

    def send(src, dst, ss, rs, device):
        copy = pltpu.make_async_remote_copy(
            src_ref=src,
            dst_ref=dst,
            send_sem=ss,
            recv_sem=rs,
            device_id=device,
            device_id_type=MESH,
        )
        copy.start()

    def all_of(ref, sem, sent=False):
        copy = pltpu.make_async_remote_copy(
            src_ref=ref,
            dst_ref=ref,
            send_sem=sem,
            recv_sem=sem,
            device_id=other,
            device_id_type=MESH,
        )
        if sent:
            copy.wait_send()
        else:
            copy.wait_recv()

    barrier = pltpu.get_barrier_semaphore()
    for r in range(1, 8):
        pl.semaphore_signal(barrier, inc=1, device_id=(dp, shard ^ r), device_id_type=MESH)
    for r in DP_ORDER:
        pl.semaphore_signal(barrier, inc=1, device_id=(dp ^ r, shard), device_id_type=MESH)

    def w_rows(a, row, side, start=0, size=None):
        n = WEIGHT_ROWS[a]
        at = pl.multiple_of((row * 2 + side) * n + start, 16)
        return weights[a].at[pl.ds(at, n if size is None else size)]

    ids_copy = pltpu.make_async_copy(ids_in, own_ids, local_sem.at[9])
    ids_copy.start()
    own_weights = []
    for a, src in enumerate((wq_in, wk_in, wv_in)):
        copy = pltpu.make_async_copy(src, w_rows(a, y, core), local_sem.at[a])
        copy.start()
        own_weights.append(copy)
    loads = []
    for n, (src, dst) in enumerate(((cache_in, cache), (tok_in, tok), (cot_in, cot))):
        copy = pltpu.make_async_copy(src, dst, local_sem.at[3 + n])
        copy.start()
        loads.append(copy)

    ids_copy.wait()
    pl.semaphore_wait(barrier, 22)

    row_lane = lax.broadcasted_iota(jnp.int32, (8, 128), 1)
    own_row = jnp.zeros((8, 128), jnp.int32)
    for k in range(8):
        own_row = jnp.where(row_lane == shard * 8 + k, own_ids[k % 2, k // 2], own_row)
    id_row[...] = own_row
    ids_shard[shard] = own_row
    for r in range(1, 8):
        send(id_row, ids_shard.at[shard], id_sem.at[0], id_sem.at[1], (dp, shard ^ r))
    all_of(ids_shard.at[0:7], id_sem.at[1])
    group = ids_shard[0]
    for s in range(1, 8):
        group = group + ids_shard[s]
    id_group[...] = group
    ids_dp[dp] = group
    for r in DP_ORDER:
        send(id_group, ids_dp.at[dp], id_sem.at[2], id_sem.at[3], (dp ^ r, shard))

    up, down, far = (y + 1) % 4, (y + 3) % 4, (y + 2) % 4
    for copy in own_weights:
        copy.wait()
    ring = {0: 0, 1: 1, 3: 2, 4: 3}

    def send_weights(kind, row, device, part=None):
        for a in range(3):
            n, cut = WEIGHT_ROWS[a], WEIGHT_CUTS[a]
            start, size = ((0, n), (0, cut), (cut, n - cut))[0 if part is None else 1 + part]
            ref = w_rows(a, row, core, start, size)
            send(ref, ref, w_send.at[kind // 4 % 2], w_recv.at[ring.get(kind, 4)], device)

    def arrived(kind):
        all_of(wq.at[0:480] if kind < 2 else wq.at[0:240], w_recv.at[ring[kind]])

    send_weights(0, y, (dp, up * 2 + core))
    send_weights(1, y, (dp, down * 2 + core))
    send_weights(2, y, other)

    lane = lax.broadcasted_iota(jnp.int32, (16, 128), 1)
    owners = lax.broadcasted_iota(jnp.int32, (16, 128), 0)
    mine = jnp.where((lane < 64) & ((group[0:1] >> 7) == owners), 1, 0)
    places = jnp.where(mine > 0, owners * 8 + running_count(mine, lane) - 1, 0)
    slots = places[0:1]
    for o in range(1, 16):
        slots = slots + places[o : o + 1]
    slots_v[...] = jnp.broadcast_to(slots, (8, 128))

    all_of(ids_dp.at[0:15], id_sem.at[3])
    ids = jnp.concatenate([ids_dp[g][0:1] for g in range(16)], axis=0)
    wanted = jnp.where((lane < 64) & ((ids >> 7) == dp), 1, 0)
    asked_v[...] = packed_left(wanted, ids & 127, lane)
    to_scalar = [
        pltpu.make_async_copy(asked_v, asked_s, local_sem.at[6]),
        pltpu.make_async_copy(slots_v, slots_s, local_sem.at[7]),
    ]
    for copy in to_scalar:
        copy.start()
    loads[0].wait()
    for copy in to_scalar:
        copy.wait()

    @pl.loop(0, 16)
    def _(g):
        for j in range(8):
            row = asked_s[g, j]
            for c, (at, width) in enumerate(CHUNKS):
                outgoing[c][g, j] = cache[row, :, at : at + width]

    for c in range(len(CHUNKS)):
        own = pl.ds(pl.multiple_of(dp * 8, 8), 8)
        for r in DP_ORDER:
            send(
                outgoing[c].at[dp ^ r], replies[c].at[own], dp_send, dp_recv.at[c], (dp ^ r, shard)
            )
    for c in range(len(CHUNKS)):
        replies[c][pl.ds(pl.multiple_of(dp * 8, 8), 8)] = outgoing[c][dp]

    loads[1].wait()
    loads[2].wait()

    @pl.loop(0, 8)
    def _(i):
        rows = pl.ds(pl.multiple_of(i * 32, 32), 32)
        t = tok[rows, :].astype(jnp.float32)
        inverse = lax.rsqrt(jnp.mean(t * t, axis=-1, keepdims=True) + 1e-06)
        normed[rows, :] = (t * inverse).astype(jnp.bfloat16)

    eye_wide = one_hot(256, 256, lambda r, c: r == c)

    @pl.loop(0, 8)
    def _(i):
        cols = pl.ds(pl.multiple_of(i * 256, 256), 256)
        normed_t[cols, :] = nt_dot(eye_wide, normed[:, cols]).astype(jnp.bfloat16)

    def hand_on(c):
        at, width = CHUNKS[c]
        all_of(replies[c].at[0:120], dp_recv.at[c])

        @pl.loop(0, 8)
        def _(s):
            for i in range(8):
                chosen[c][s, i] = replies[c][slots_s[0, s * 8 + i]]

        for r in range(1, 8):
            send(
                chosen[c].at[shard ^ r],
                lat.at[:, shard, :, pl.ds(at, width)],
                sh_send,
                sh_recv.at[c],
                (dp, shard ^ r),
            )
        lat[:, shard, :, at : at + width] = chosen[c][shard]

    def project(at, width):
        @pl.loop(0, CH_DEV)
        def _(n):
            block = lat[pl.ds(2 * n, 2), :, :, at : at + width].reshape(256, width)
            rows = pl.ds(pl.multiple_of((n & 1) * 16, 16), 16)
            for w, total in ((wk, acc), (wv, value_part)):
                for j in range(0, 8, 2):
                    r = nn_dot(block, w[at : at + width, 128 * j : 128 * j + 256])
                    for e in range(2):
                        tile = r[:, 128 * e : 128 * e + 128].reshape(16, 16, 128)
                        index = (n >> 1) * 8 + j + e
                        if at > 0:
                            tile = tile + total[index, rows]
                        total[index, rows] = tile

    def landed(c):
        all_of(replies[c].at[0:56], sh_recv.at[c])

    arrived(0)
    send_weights(3, down, (dp, up * 2 + core), 0)
    send_weights(5, down, other)
    arrived(1)
    send_weights(4, up, (dp, down * 2 + core), 1)
    send_weights(6, up, other)
    hand_on(0)
    hand_on(1)
    arrived(3)
    send_weights(7, far, other, 0)
    arrived(4)
    send_weights(8, far, other, 1)
    hand_on(2)
    all_of(wq.at[0:1920], w_recv.at[4])

    scale = HEAD_DIM ** (-0.5)

    @pl.loop(0, 4)
    def _(i):
        cols = pl.ds(pl.multiple_of(i * 256, 256), 256)
        q[:, cols] = (nn_dot(normed[...], wq[:, cols]) * scale).astype(jnp.bfloat16)

    def turn_latents(b):
        at, width = ((0, 256), (128, 384), (384, 384), (640, 256))[b]
        pick = one_hot(
            256,
            width,
            lambda r, c: (c + at == 224 * b + 7 * (r >> 3) + (r & 7)) & ((r & 7) < 7),
        )
        for n in range(4):
            block = lat[2 * n : 2 * n + 2, :, :, at : at + width].reshape(256, width)
            lat_t[256 * b : 256 * b + 256, 256 * n : 256 * n + 256] = nt_dot(pick, block).astype(
                jnp.bfloat16
            )

    landed(0)
    project(0, 384)
    turn_latents(0)
    hand_on(3)
    landed(1)
    turn_latents(1)
    hand_on(4)
    landed(2)
    project(384, 256)
    landed(3)
    project(640, 128)
    turn_latents(2)
    landed(4)
    turn_latents(3)

    eye = one_hot(128, 128, lambda r, c: r == c)
    zero = jnp.zeros((SPAN, HEAD_DIM), jnp.bfloat16)

    def diagonal(ref, rows, at):
        a = ref[rows, at : at + HEAD_DIM]
        b = ref[rows, at + HEAD_DIM : at + 2 * HEAD_DIM]
        return jnp.concatenate(
            [jnp.concatenate([a, zero], axis=1), jnp.concatenate([zero, b], axis=1)], axis=0
        )

    def project_last(w, total, c, at):
        block = lat[2 * c : 2 * c + 2, :, :, 768:LAT].reshape(256, 128)
        r = nn_dot(block, w[768:LAT, at : at + 256])
        tiles = [
            total[(c >> 1) * 8 + at // 128 + e, 16 * (c & 1) : 16 * (c & 1) + 16].reshape(256, 128)
            for e in range(2)
        ]
        return (jnp.concatenate(tiles, axis=1) + r).astype(jnp.bfloat16)

    def attend(at):
        mid = at + HEAD_DIM
        end = at + 256
        for c in range(CH_DEV):
            rows = slice(256 * c, 256 * c + 256)
            trows = slice(SPAN * c, SPAN * c + SPAN)
            kp = project_last(wk, acc, c, at)
            vp = project_last(wv, value_part, c, at)
            q2 = diagonal(q, trows, at)
            g2 = diagonal(cot, trows, at)
            scores = nt_dot(kp, q2)
            e = jnp.exp(scores - jnp.max(scores, axis=0, keepdims=True))
            prob = e * (1.0 / jnp.sum(e, axis=0, keepdims=True))
            prob_t = prob.astype(jnp.bfloat16)
            prob_r = nt_dot(eye, prob_t).astype(jnp.bfloat16)
            c2 = nn_dot(prob_r, vp).astype(jnp.bfloat16)
            ctx[trows, at:mid] = c2[:SPAN, :HEAD_DIM]
            ctx[trows, mid:end] = c2[SPAN:, HEAD_DIM:]
            vg[rows, :] = nn_dot(prob_t, g2).astype(jnp.bfloat16)
            pg = nt_dot(vp, g2)
            sg_t = (prob * (pg - jnp.sum(prob * pg, axis=0, keepdims=True))).astype(jnp.bfloat16)
            kg[rows, :] = nn_dot(sg_t, q2).astype(jnp.bfloat16)
            sg = nt_dot(eye, sg_t).astype(jnp.bfloat16)
            qg2 = (nn_dot(sg, kp) * scale).astype(jnp.bfloat16)
            qg[trows, :HEAD_DIM] = qg2[:SPAN, :HEAD_DIM]
            qg[trows, HEAD_DIM:] = qg2[SPAN:, HEAD_DIM:]

    def across(dims):
        pz, px, py = z, x, y
        for d in dims:
            if d < 2:
                pz = flip(pz, d % 2 == 0)
            elif d < 4:
                px = flip(px, d % 2 == 0)
            else:
                py = flip(py, d % 2 == 0)
        return (pz * 4 + px, py * 2 + core)

    chip = z * 16 + x * 4 + y

    def to_other_core(t):
        send(xs.at[t, 1 - core], crecv.at[t], send_sem.at[0], core_recv.at[t // 2], other)

    def eight(t, second):
        code = place(chip, t & 1)
        high = (t & 1 == 0) != second
        devices = {}
        for m in (7, 6, 5, 3, 4, 2, 1):
            dims = [2 * e + (0 if high else 1) for e in range(3) if m & (4 >> e)]
            devices[m] = across(dims)
        return (code & 7 if second else code >> 3), devices

    def exchange_first(t):
        if t % 2 == 0:
            all_of(crecv.at[0:2], core_recv.at[t // 2])

        def summed(at, step):
            where = pl.ds(at, step)
            return xs[t, core, where].astype(jnp.float32) + crecv[t, where].astype(jnp.float32)

        @pl.loop(0, 4)
        def _(i):
            snd[t, pl.ds(i * 16, 16)] = summed(i * 16, 16).astype(jnp.bfloat16)

        own, devices = eight(t, False)
        for m, device in devices.items():
            send(
                snd.at[t, pl.ds((own ^ m) * 8, 8)],
                rcv.at[t, pl.ds(8 * m, 8)],
                send_sem.at[1],
                first_recv.at[t],
                device,
            )
        acc[t, pl.ds(0, 8)] = summed(own * 8, 8)

    def exchange_second(t):
        all_of(rcv.at[t, 8:64], first_recv.at[t])
        whole = acc[t, pl.ds(0, 8)]
        for m in range(1, 8):
            whole = whole + rcv[t, pl.ds(8 * m, 8)].astype(jnp.float32)
        acc[t, pl.ds(0, 8)] = whole
        snd[t, pl.ds(64, 8)] = whole.astype(jnp.bfloat16)
        own, devices = eight(t, True)
        for m, device in devices.items():
            send(
                snd.at[t, 64 + (own ^ m)],
                rcv.at[t, m],
                send_sem.at[2],
                second_recv.at[t // 2],
                device,
            )

    def finish(t):
        if t % 2 == 0:
            all_of(rcv.at[0:2, 1:8], second_recv.at[t // 2])
        total = acc[t, place(chip, t & 1) & 7]
        for m in range(1, 8):
            total = total + rcv[t, m].astype(jnp.float32)
        at = 128 * (t % 8)
        grads[16 * (t // 8) : 16 * (t // 8) + 16, at : at + 128] = total

    def query_sums(n):
        @pl.loop(0, 4)
        def _(i):
            turned = normed_t[pl.ds(pl.multiple_of(i * 512, 512), 512), :]
            r = nn_dot(turned, qg[...]).astype(jnp.bfloat16)
            start = [place(16 * i, e) for e in range(2)]
            for j in range(32):
                for e in range(2):
                    t = 2 * n + e
                    xs[t, j & 1, start[e] ^ place(j >> 1, e)] = r[
                        16 * j : 16 * j + 16, 128 * e : 128 * e + 128
                    ]

        to_other_core(2 * n)
        to_other_core(2 * n + 1)

    def latent_sums(n):
        for b in range(2):
            turned = lat_t[512 * b : 512 * b + 512, :]
            rk = nn_dot(turned, kg[...])
            rv = nn_dot(turned, vg[...])
            start = [place(32 * b, e) for e in range(2)]
            for j in range(64):
                both = jnp.concatenate([rk[8 * j : 8 * j + 8], rv[8 * j : 8 * j + 8]], axis=0)
                both = both.astype(jnp.bfloat16)
                for e in range(2):
                    t = 8 + 2 * n + e
                    xs[t, j & 1, start[e] ^ place(j >> 1, e)] = both[
                        :, 128 * e : 128 * e + 128
                    ]

        to_other_core(8 + 2 * n)
        to_other_core(9 + 2 * n)

    def parts(n):
        return (2 * n, 2 * n + 1, 8 + 2 * n, 9 + 2 * n)

    for n in range(4):
        attend(256 * n)
        if n == 3:
            ctx_copy = pltpu.make_async_copy(ctx, ctx_out, local_sem.at[8])
            ctx_copy.start()
        if n > 0:
            for t in parts(n - 1):
                exchange_first(t)
        query_sums(n)
        latent_sums(n)
        if n == 2:
            for t in parts(0):
                exchange_second(t)
    for t in parts(3):
        exchange_first(t)
    for n in (1, 2, 3):
        for t in parts(n):
            exchange_second(t)
    for t in range(16):
        finish(t)
    ctx_copy.wait()
    for ref, sem in (
        (ids_shard.at[0:7], id_sem.at[0]),
        (ids_dp.at[0:15], id_sem.at[2]),
        (wq.at[0:1920], w_send.at[0]),
        (wq.at[0:1440], w_send.at[1]),
        (cache.at[0:120], dp_send),
        (cache.at[0:56], sh_send),
        (crecv, send_sem.at[0]),
        (snd.at[:, 0:56], send_sem.at[1]),
        (snd.at[:, 0:7], send_sem.at[2]),
    ):
        all_of(ref, sem, sent=True)


def emit_kernel(ctx, grads, ctx_out, gq, gk, gv):
    ctx_out[...] = ctx[...]
    gq[...] = grads[0:16]
    gk[...] = grads[16:23]
    gv[...] = grads[24:31]


def body(tokens, ctx_cotangent, latent_cache, nbr_ids, w_query, w_key, w_value):
    f32, bf, i32 = jnp.float32, jnp.bfloat16, jnp.int32
    vmem = pl.BlockSpec(memory_space=pltpu.VMEM)
    hbm = pl.BlockSpec(memory_space=pl.ANY)
    dma = pltpu.SemaphoreType.DMA
    widths = [w for _, w in CHUNKS]
    context, grads = pl.pallas_call(
        whole_kernel,
        out_shape=(
            jax.ShapeDtypeStruct((256, INNER), bf),
            jax.ShapeDtypeStruct((32, INNER), f32),
        ),
        in_specs=[hbm] * 7,
        out_specs=(hbm, vmem),
        scratch_shapes=[
            pltpu.SMEM((2, 4), i32),
            pltpu.VMEM((8, 128), i32),
            pltpu.VMEM((8, 8, 128), i32),
            pltpu.VMEM((8, 128), i32),
            pltpu.VMEM((16, 8, 128), i32),
            pltpu.VMEM((16, 128), i32),
            pltpu.VMEM((8, 128), i32),
            pltpu.SMEM((16, 128), i32),
            pltpu.SMEM((8, 128), i32),
            pltpu.VMEM((128, 16, LAT), bf),
            pltpu.VMEM((256, D), bf),
            pltpu.VMEM((256, INNER), bf),
            pltpu.VMEM((D, INNER), bf),
            pltpu.VMEM((LAT, INNER), bf),
            pltpu.VMEM((LAT, INNER), bf),
            *(pltpu.VMEM((16, 8, 16, w), bf) for w in widths),
            *(pltpu.VMEM((128, 16, w), bf) for w in widths),
            *(pltpu.VMEM((8, 8, 16, w), bf) for w in widths),
            pltpu.VMEM((8, 8, 16, LAT), bf),
            pltpu.VMEM((256, D), bf),
            pltpu.VMEM((D, 256), bf),
            pltpu.VMEM((256, INNER), bf),
            pltpu.VMEM((256, 256), bf),
            pltpu.VMEM((1024, 256), bf),
            pltpu.VMEM((1024, 256), bf),
            pltpu.VMEM((1024, 1024), bf),
            pltpu.VMEM((256, INNER), bf),
            pltpu.VMEM((16, 2, CHIPS, 16, 128), bf),
            pltpu.VMEM((16, CHIPS, 16, 128), bf),
            pltpu.VMEM((16, CHIPS // 2, 16, 128), f32),
            pltpu.VMEM((16, CHIPS + 8, 16, 128), bf),
            pltpu.VMEM((16, CHIPS, 16, 128), bf),
            pltpu.VMEM((16, CHIPS // 2, 16, 128), f32),
            dma((10,)),
            dma((4,)),
            dma((2,)),
            dma((5,)),
            dma,
            dma((5,)),
            dma,
            dma((5,)),
            dma((3,)),
            dma((8,)),
            dma((16,)),
            dma((8,)),
        ],
        compiler_params=pltpu.CompilerParams(
            collective_id=1, has_side_effects=True, vmem_limit_bytes=67043328
        ),
        name="retro",
    )(
        nbr_ids.T,
        tokens,
        ctx_cotangent,
        latent_cache,
        w_query,
        w_key,
        w_value,
    )
    return pl.pallas_call(
        emit_kernel,
        out_shape=(
            jax.ShapeDtypeStruct((256, INNER), bf),
            jax.ShapeDtypeStruct((16, INNER), f32),
            jax.ShapeDtypeStruct((7, INNER), f32),
            jax.ShapeDtypeStruct((7, INNER), f32),
        ),
        in_specs=[vmem] * 2,
        out_specs=(vmem,) * 4,
        name="emit",
    )(context, grads)


def solution(mesh):
    return jax.shard_map(
        body,
        mesh=mesh,
        in_specs=(
            P(("dp", "shard"), None),
            P(("dp", "shard"), None),
            P("dp", "shard", None),
            P(("dp", "shard"), None),
            P("shard", None),
            P("shard", None),
            P("shard", None),
        ),
        out_specs=(
            P(("dp", "shard"), None),
            P(("dp", "shard"), None),
            P(("dp", "shard"), None),
            P(("dp", "shard"), None),
        ),
        check_vma=False,
    )
```
